512 devices in a mesh: tiles: 32 (over z, core), feat: 16 (over y, x).
Axes of the slice: x: 4, y: 4, z: 16, core: 2. Of those that a mesh axis runs over, the one named last changes fastest.
Arguments:
- feats: bfloat16 [1024, 256, 128], P('tiles', 'feat'), may hold values from -6 to 6
- weight: bfloat16 [128, 128], P('feat'), may hold values from -0.5 to 0.5
- bias: float32 [128], replicated, may hold values from -3 to 3
- neighbours: int32 [1024, 16], P('tiles'), may hold values from 0 to 1023, as said below
- counts: int32 [1024], P('tiles'), may hold values from 4 to 16, as said below
- adj_words: int32 [1024, 16, 24, 256], P('tiles', 'feat'), may hold values from 0 to 2047, as said below
- tile_row: int32 [1024], replicated, may hold values from 0 to 1023, as said below
Outputs:
- new_feats: bfloat16 [1024, 256, 128], P('tiles', 'feat')
The draws below stay inside these ranges and needn't reach their ends.
Inputs may be any that keep to these rules, and one draw needn't show every extreme that they name: A permutation of the slide's tiles; slide tile s is stored in the same band as its id, tile_row[s] // 32 == s // 32. Slide ids run row by row over a grid of 8 tile columns. If tile_row[s] == r, every neighbours[r, k] lies within 2 grid rows and 2 grid columns of s (grid row = id // 8, column = id % 8). Slots at or past counts[r] hold valid ids that are not used. `counts`: some tile has all 16 slots live in every draw. `adj_words`: word w holds source cells 11 w to 11 w + 10 in its bits 0 to 10; bits for cells 256 and beyond are zero.
All inputs are finite; a program needn't handle non-finite values.
Results may differ from the reference program's by a relative error of at most 0.0031.
Values may be sent and summed in bfloat16 or wider, within the bound.
A program may use at most 64 MiB of HBM per device.

```python
import jax
import jax.numpy as jnp
import numpy as np
from jax import lax

CELLS = 256
FEAT = 128
SLOTS = 16
GRID_COLS = 8
TPD = 32
WORDS = 24
NTILES = 1024


def band_order(key):
    slide = jnp.arange(NTILES, dtype=jnp.int32)
    noise = jax.random.randint(jax.random.fold_in(key, 3), (NTILES,), 0, 1024)
    score = slide // TPD * (1024 * NTILES) + noise * NTILES + slide
    return jnp.argsort(score, stable=True).astype(jnp.int32)


def draw_tile_row(key, part):
    order = band_order(key)
    return jnp.argsort(order, stable=True).astype(jnp.int32)


def draw_neighbours(key, part):
    order = band_order(key)
    pairs = [(a, b) for a in range(-2, 3) for b in range(-2, 3) if a != 0 or b != 0]
    row_steps = jnp.asarray(np.array([p[0] for p in pairs], dtype=np.int32))
    col_steps = jnp.asarray(np.array([p[1] for p in pairs], dtype=np.int32))
    grid_rows = NTILES // GRID_COLS
    grid_row = order // GRID_COLS
    grid_col = order % GRID_COLS
    score = jax.random.randint(jax.random.fold_in(key, 5), (NTILES, 24), 0, 1024) * 32 + jnp.arange(24, dtype=jnp.int32)[None, :]
    picked = jnp.argsort(score, axis=1, stable=True)[:, :SLOTS]
    near_row = jnp.clip(grid_row[:, None] + row_steps[picked], 0, grid_rows - 1)
    near_col = jnp.clip(grid_col[:, None] + col_steps[picked], 0, GRID_COLS - 1)
    return (near_row * GRID_COLS + near_col).astype(jnp.int32)


def draw_counts(key, part):
    bands = NTILES // TPD
    level = jax.random.randint(jax.random.fold_in(key, 11), (bands,), 0, 4)
    forced = jax.random.randint(jax.random.fold_in(key, 12), (), 0, bands)
    level = jnp.where(jnp.arange(bands, dtype=jnp.int32) == forced, 3, level)
    rows = jnp.arange(NTILES, dtype=jnp.int32)
    tile_level = level[rows // TPD]
    extra = jax.random.randint(jax.random.fold_in(key, 13), (NTILES,), 0, 4 * tile_level + 1)
    total = jnp.minimum(4 + extra, SLOTS)
    spot = forced * TPD + jax.random.randint(jax.random.fold_in(key, 14), (), 0, TPD)
    return jnp.where(rows == spot, SLOTS, total).astype(jnp.int32)


def draw_adj_words(key, part):
    shape = (NTILES, SLOTS, WORDS, CELLS)
    base = jax.random.fold_in(key, 21)
    packed = jax.random.randint(jax.random.fold_in(base, 0), shape, 0, 1 << 11)
    packed = packed & jax.random.randint(jax.random.fold_in(base, 1), shape, 0, 1 << 11)
    packed = packed & jax.random.randint(jax.random.fold_in(base, 2), shape, 0, 1 << 11)
    packed = packed & jax.random.randint(jax.random.fold_in(base, 3), shape, 0, 1 << 11)
    remain = CELLS - 11 * (WORDS - 1)
    limit = jnp.where(jnp.arange(WORDS, dtype=jnp.int32) == WORDS - 1, (1 << remain) - 1, (1 << 11) - 1)
    return (packed & limit[:, None]).astype(jnp.int32)


def levels(stream_key, shape, pieces, least, top_value):
    def one(position, blocks):
        steps = jax.random.uniform(jax.random.fold_in(jax.random.fold_in(stream_key, 6), position), (blocks,), jnp.float32, least / len(pieces), top_value / len(pieces))
        return jnp.repeat(jnp.exp(steps), shape[position] // blocks).reshape((-1,) + (1,) * (len(shape) - position - 1))

    gain = one(*pieces[0])
    for cut in pieces[1:]:
        gain = gain * one(*cut)
    return gain


def normal_values(rng, shape, deviation, reach, pieces=(), kind=jnp.bfloat16):
    values = jax.random.normal(rng, shape, jnp.float32) * deviation
    if len(pieces) > 0:
        values = levels(rng, shape, pieces, -0.22, 0.18) * values
    return jnp.clip(values, min=-reach, max=reach).astype(kind)


def setup_inputs(seed: int = 0) -> dict:
    arg_keys = jax.random.split(jax.random.key(seed), 8)
    feats = normal_values(arg_keys[0], (NTILES, CELLS, FEAT), 1.0, 6.0, ((0, 32), (1, 16)))
    weight = normal_values(arg_keys[1], (FEAT, FEAT), FEAT ** -0.5, 0.5, ((0, 16),))
    bias = normal_values(arg_keys[2], (FEAT,), 0.5, 3.0, (), jnp.float32)
    neighbours = draw_neighbours(jax.random.fold_in(arg_keys[7], 71), 0)
    counts = draw_counts(jax.random.fold_in(arg_keys[7], 71), 0)
    adj_words = draw_adj_words(jax.random.fold_in(arg_keys[7], 71), 0)
    tile_row = draw_tile_row(jax.random.fold_in(arg_keys[7], 71), 0)
    return {"feats": feats, "weight": weight, "bias": bias, "neighbours": neighbours, "counts": counts, "adj_words": adj_words, "tile_row": tile_row}


def unpack_bits(packed):
    shifts = jnp.arange(11, dtype=jnp.int32)
    bit_values = packed[:, :, None, :] >> shifts[None, None, :, None] & 1
    unrolled = bit_values.reshape(packed.shape[0], packed.shape[1] * 11, packed.shape[2])
    return unrolled[:, :CELLS, :].astype(jnp.float32)

def reference(feats, weight, bias, neighbours, counts, adj_words, tile_row):
    source = tile_row[neighbours].astype(jnp.int32)
    live_slots = (jnp.arange(SLOTS, dtype=jnp.int32)[None, :] < counts[:, None]).astype(jnp.float32)

    def one_tile(inputs):
        rows, live_row, packed = inputs
        mask_block = unpack_bits(packed) * live_row[:, None, None]
        gathered = feats[rows].astype(jnp.float32)
        summed = jnp.einsum('kjd,kjf->df', mask_block, gathered)
        degree = lax.optimization_barrier(jnp.sum(mask_block, axis=(0, 1)))
        return (summed, degree)
    summed, degree = lax.map(one_tile, (source, live_slots, adj_words), batch_size=8)
    base = feats.astype(jnp.float32)
    normed = ((summed + base) / jnp.sqrt(degree + 1.0)[:, :, None]).astype(jnp.bfloat16)
    linear = jnp.dot(normed.reshape(-1, FEAT), weight, preferred_element_type=jnp.float32) + bias
    result = base.reshape(-1, FEAT) + jax.nn.relu(linear)
    return result.astype(jnp.bfloat16).reshape(NTILES, CELLS, FEAT)
```

```python
import functools

import jax
import jax.numpy as jnp
from jax import lax
from jax.experimental import pallas as pl
from jax.experimental.pallas import tpu as pltpu
from jax.sharding import PartitionSpec as P

MESH = pl.DeviceIdType.MESH
BF16 = jnp.bfloat16
F32 = jnp.float32
I32 = jnp.int32

SLOTS = 16
CELLS = 256
CHUNK = 16
WORDS = 24
BITS = 11
LANES = 128
TILES = 32
WIN_ROWS = 5
WIN_COLS = 6


def kernel(
    n_tiles,
    feats_hbm, weight_hbm, bias_ref, nb_hbm, words_hbm, counts_ref, rows_ref,
    out_ref,
    feats_v, words_v, weight_v, nb_own, nb_other, stage_f, stage_w, win, wbuf, wall, bits32, mask, feats_t, stage_o, obuf, inverse,
    local_sem, nb_send, nb_sem, word_send, word_sem, weight_send, weight_sem, win_send, win_sem, fwd_send, fwd_sem, out_send, out_sem,
):
    t = lax.axis_index("tiles")
    f = lax.axis_index("feat")
    z = t // 2
    core = t % 2
    partner = 2 * z + 1 - core
    row_in_plane = f // 2
    half = f % 2
    home = f // 8
    dest_row = 8 * z + row_in_plane
    n_planes = n_tiles // 2

    def device(tiles, feat):
        return {"tiles": tiles, "feat": feat}

    loads = [
        pltpu.make_async_copy(words_hbm, words_v, local_sem.at[0]),
        pltpu.make_async_copy(feats_hbm, feats_v, local_sem.at[1]),
        pltpu.make_async_copy(weight_hbm, weight_v, local_sem.at[2]),
        pltpu.make_async_copy(nb_hbm, nb_own, local_sem.at[3]),
    ]
    for load in loads:
        load.start()

    barrier = pltpu.get_barrier_semaphore()

    def greet(i, carry):
        tiles, feat = 2 * z + i // 16, i % 16

        @pl.when(jnp.logical_or(tiles != t, feat != f))
        def _():
            pl.semaphore_signal(barrier, inc=1, device_id=device(tiles, feat), device_id_type=MESH)

        return carry

    lax.fori_loop(0, 32, greet, 0)

    needs_before = jnp.logical_and(row_in_plane < 2, z > 0)
    needs_after = jnp.logical_and(row_in_plane >= 6, z < n_planes - 1)

    def greet_halo(tiles):
        def body(i, carry):
            pl.semaphore_signal(barrier, inc=1, device_id=device(tiles, core * 8 + i), device_id_type=MESH)
            return carry

        lax.fori_loop(0, 8, body, 0)

    @pl.when(needs_before)
    def _():
        greet_halo(2 * z - 1)

    @pl.when(needs_after)
    def _():
        greet_halo(2 * z + 2)

    for load in loads:
        load.wait()

    def order(s, carry):
        row = jnp.clip(rows_ref[t * TILES + s] - t * TILES, 0, TILES - 1)
        live = f < counts_ref[row]
        w = words_v[row]
        packed = w[:, :LANES] | (w[:, LANES:] << 16)
        stage_w[s] = jnp.where(live, packed, jnp.zeros_like(packed))
        stage_f[s // 8, s % 8] = feats_v[row]
        return carry

    lax.fori_loop(0, TILES, order, 0)

    sends_beyond = jnp.logical_or(
        jnp.logical_and(core == 1, z < n_planes - 1), jnp.logical_and(core == 0, z > 0)
    )

    @pl.when(sends_beyond)
    def _():
        pl.semaphore_wait(barrier, 35)

    @pl.when(jnp.logical_not(sends_beyond))
    def _():
        pl.semaphore_wait(barrier, 31)

    nb_copy = pltpu.make_async_remote_copy(
        nb_own, nb_other, nb_send, nb_sem, device_id=device(partner, f), device_id_type=MESH
    )
    nb_copy.start()

    def word_copy(i):
        chip = core * 8 + (i // 2 + f) % 8
        side = i % 2
        first = 4 * (chip % 8) + 2 * side
        mine = jnp.logical_and(chip == f, side == core)
        copy = pltpu.make_async_remote_copy(
            stage_w.at[pl.ds(first, 2)], wbuf.at[f], word_send.at[i], word_sem.at[f],
            device_id=device(2 * z + side, chip), device_id_type=MESH,
        )
        return copy, mine, first

    def start_words(i, carry):
        copy, mine, first = word_copy(i)

        @pl.when(jnp.logical_not(mine))
        def _():
            copy.start()

        @pl.when(mine)
        def _():
            wbuf[f] = stage_w[pl.ds(first, 2)]

        return carry

    lax.fori_loop(0, 16, start_words, 0)

    weight_mine = weight_v[...]
    wall[f] = weight_mine

    def weight_copy(i):
        chip = (f + i) % 16
        return pltpu.make_async_remote_copy(
            weight_v, wall.at[f], weight_send.at[i], weight_sem.at[f],
            device_id=device(t, chip), device_id_type=MESH,
        )

    def start_weight(i, carry):
        weight_copy(i).start()
        return carry

    lax.fori_loop(1, 16, start_weight, 0)

    my_cells = pl.ds(pl.multiple_of(f * CHUNK, CHUNK), CHUNK)

    def feat_copy(i):
        combo = (i // 4 + row_in_plane) % 10
        step = combo // 2 - 2
        h = combo % 2
        r = i % 4
        to_row = 4 * t + r + step
        valid = jnp.logical_and(to_row >= 0, to_row < 4 * n_tiles)
        tiles = 2 * (to_row // 8) + f // 8
        chip = 2 * (to_row % 8) + h
        mine = jnp.logical_and(tiles == t, chip == f)
        copy = pltpu.make_async_remote_copy(
            stage_f.at[r, pl.ds(2 * h, WIN_COLS)],
            win.at[2 - step, :, my_cells],
            win_send.at[i], win_sem.at[2 - step, f % 8],
            device_id=device(tiles, chip), device_id_type=MESH,
        )
        return copy, valid, mine, r, h, step

    def start_feats(i, carry):
        copy, valid, mine, r, h, step = feat_copy(i)

        @pl.when(jnp.logical_and(valid, jnp.logical_not(mine)))
        def _():
            copy.start()

        @pl.when(jnp.logical_and(valid, mine))
        def _():
            win[2 - step, :, my_cells] = stage_f[r, pl.ds(2 * h, WIN_COLS)]

        return carry

    lax.fori_loop(0, 40, start_feats, 0)

    def invert(r, carry):
        def look(s, found):
            return found + jnp.where(rows_ref[t * TILES + s] == t * TILES + r, s, 0)

        inverse[r] = jnp.clip(lax.fori_loop(0, TILES, look, 0), 0, TILES - 1)
        return carry

    lax.fori_loop(0, TILES, invert, 0)

    def row_exists(w):
        row = dest_row + w - 2
        return jnp.logical_and(row >= 0, row < 4 * n_tiles)

    def clear(w, carry):
        @pl.when(jnp.logical_not(row_exists(w)))
        def _():
            win[w] = jnp.zeros((WIN_COLS, CELLS, LANES), BF16)

        return carry

    lax.fori_loop(0, WIN_ROWS, clear, 0)

    ones_rows = jnp.ones((16, CELLS), BF16)

    def fill_ones(i, carry):
        feats_t[i, pl.ds(LANES, 16)] = ones_rows
        return carry

    lax.fori_loop(0, WIN_ROWS * WIN_COLS, fill_ones, 0)

    def unpack(k, carry):
        @pl.when(jnp.logical_not(jnp.logical_and(k == f, core == home)))
        def _():
            pltpu.make_async_copy(wbuf.at[k], wbuf.at[k], word_sem.at[k]).wait()

        for tile in range(2):
            packed = wbuf[k, tile]
            for b in range(BITS):
                bits32[0, pl.ds(b, WORDS, stride=BITS), :] = (packed >> b) & 1
                bits32[1, pl.ds(b, WORDS, stride=BITS), :] = (packed >> (16 + b)) & 1
            mask[tile, k, :, :LANES] = bits32[0, :CELLS].astype(F32).astype(BF16)
            mask[tile, k, :, LANES:] = bits32[1, :CELLS].astype(F32).astype(BF16)
        return carry

    lax.fori_loop(0, SLOTS, unpack, 0)

    kept = pl.ds(pl.multiple_of(core * LANES, LANES), LANES)

    def forward_copy(w):
        return pltpu.make_async_remote_copy(
            win.at[w, :, kept], win.at[w, :, kept], fwd_send.at[w], fwd_sem.at[w],
            device_id=device(partner, f), device_id_type=MESH,
        )

    def forward(w, carry):
        @pl.when(row_exists(w))
        def _():
            local = jnp.logical_and(home == core, (dest_row + w - 2) // 4 == t)

            def arrive(i, c):
                @pl.when(jnp.logical_not(jnp.logical_and(local, i == f % 8)))
                def _():
                    cells = pl.ds(pl.multiple_of((core * 8 + i) * CHUNK, CHUNK), CHUNK)
                    pltpu.make_async_copy(
                        win.at[w, :, cells], win.at[w, :, cells], win_sem.at[w, i]
                    ).wait()

                return c

            lax.fori_loop(0, 8, arrive, 0)
            forward_copy(w).start()

        return carry

    lax.fori_loop(0, WIN_ROWS, forward, 0)

    def turn(w, carry):
        @pl.when(row_exists(w))
        def _():
            forward_copy(w).wait_recv()

        for c in range(WIN_COLS):
            feats_t[w * WIN_COLS + c, pl.ds(0, LANES)] = win[w, c].T
        return carry

    lax.fori_loop(0, WIN_ROWS, turn, 0)

    nb_copy.wait_recv()

    def weight_wait(i, carry):
        chip = (f + i) % 16
        pltpu.make_async_copy(wall.at[chip], wall.at[chip], weight_sem.at[chip]).wait()
        return carry

    lax.fori_loop(1, 16, weight_wait, 0)
    weight = wall[...].astype(F32).reshape(LANES, LANES).astype(BF16)
    bias = bias_ref[...]
    band = 2 * z + home

    for tile in range(2):
        slide = 4 * (f % 8) + 2 * core + tile
        row = jnp.clip(rows_ref[band * TILES + slide] - band * TILES, 0, TILES - 1)

        def add(k, acc):
            near = jnp.where(home == core, nb_own[row, k], nb_other[row, k])
            place = (near // 8 - (dest_row - 2)) * WIN_COLS + near % 8 - 2 * half
            place = jnp.clip(place, 0, WIN_ROWS * WIN_COLS - 1)
            return acc + jnp.dot(feats_t[place], mask[tile, k], preferred_element_type=F32)

        total = lax.fori_loop(0, SLOTS, add, jnp.zeros((LANES + 16, CELLS), F32)).T
        base = win[2, 4 * half + 2 * core + tile - 2 * half].astype(F32)
        degree = total[:, LANES : LANES + 1]
        normed = ((total[:, :LANES] + base) / jnp.sqrt(degree + 1.0)).astype(BF16)
        linear = jnp.dot(normed, weight, preferred_element_type=F32) + bias
        stage_o[tile] = (base + jnp.maximum(linear, 0.0)).astype(BF16)

    first_out = 4 * (f % 8) + 2 * core

    def out_copy(i):
        chip = (f + i) % 16
        cells = pl.ds(pl.multiple_of(chip * CHUNK, CHUNK), CHUNK)
        mine = jnp.logical_and(i == 0, home == core)
        copy = pltpu.make_async_remote_copy(
            stage_o.at[:, cells], obuf.at[pl.ds(first_out, 2)], out_send.at[i], out_sem.at[first_out // 2],
            device_id=device(2 * z + home, chip), device_id_type=MESH,
        )
        return copy, mine

    def start_out(i, carry):
        copy, mine = out_copy(i)

        @pl.when(jnp.logical_not(mine))
        def _():
            copy.start()

        @pl.when(mine)
        def _():
            obuf[pl.ds(first_out, 2)] = stage_o[:, my_cells]

        return carry

    lax.fori_loop(0, 16, start_out, 0)

    nb_copy.wait_send()

    def end_words(i, carry):
        copy, mine, _ = word_copy(i)

        @pl.when(jnp.logical_not(mine))
        def _():
            copy.wait_send()

        return carry

    lax.fori_loop(0, 16, end_words, 0)

    def end_weight(i, carry):
        weight_copy(i).wait_send()
        return carry

    lax.fori_loop(1, 16, end_weight, 0)

    def end_feats(i, carry):
        copy, valid, mine, _, _, _ = feat_copy(i)

        @pl.when(jnp.logical_and(valid, jnp.logical_not(mine)))
        def _():
            copy.wait_send()

        return carry

    lax.fori_loop(0, 40, end_feats, 0)

    def end_forward(w, carry):
        @pl.when(row_exists(w))
        def _():
            forward_copy(w).wait_send()

        return carry

    lax.fori_loop(0, WIN_ROWS, end_forward, 0)

    def end_out(i, carry):
        copy, mine = out_copy(i)

        @pl.when(jnp.logical_not(mine))
        def _():
            copy.wait_send()

        return carry

    lax.fori_loop(0, 16, end_out, 0)

    def arrive_out(i, carry):
        @pl.when(jnp.logical_not(jnp.logical_and(home == core, i == first_out // 2)))
        def _():
            pair = pl.ds(2 * i, 2)
            pltpu.make_async_copy(obuf.at[pair], obuf.at[pair], out_sem.at[i]).wait()

        return carry

    lax.fori_loop(0, 16, arrive_out, 0)

    def put(r, carry):
        out_ref[r] = obuf[inverse[r]]
        return carry

    lax.fori_loop(0, TILES, put, 0)


def solution(mesh):
    n_tiles = mesh.shape["tiles"]

    def per_device(feats, weight, bias, neighbours, counts, adj_words, tile_row):
        vmem = pl.BlockSpec(memory_space=pltpu.VMEM)
        smem = pl.BlockSpec(memory_space=pltpu.SMEM)
        hbm = pl.BlockSpec(memory_space=pl.ANY)
        words = adj_words.reshape(TILES, WORDS, CELLS)
        return pl.pallas_call(
            functools.partial(kernel, n_tiles),
            out_shape=jax.ShapeDtypeStruct(feats.shape, BF16),
            in_specs=[hbm, hbm, vmem, hbm, hbm, smem, smem],
            out_specs=vmem,
            scratch_shapes=[
                pltpu.VMEM((TILES, CHUNK, LANES), BF16),
                pltpu.VMEM((TILES, WORDS, CELLS), I32),
                pltpu.VMEM((8, LANES), BF16),
                pltpu.SMEM((TILES, SLOTS), I32),
                pltpu.SMEM((TILES, SLOTS), I32),
                pltpu.VMEM((4, 8, CHUNK, LANES), BF16),
                pltpu.VMEM((TILES, WORDS, LANES), I32),
                pltpu.VMEM((WIN_ROWS, WIN_COLS, CELLS, LANES), BF16),
                pltpu.VMEM((SLOTS, 2, WORDS, LANES), I32),
                pltpu.VMEM((16, 8, LANES), BF16),
                pltpu.VMEM((2, WORDS * BITS, LANES), I32),
                pltpu.VMEM((2, SLOTS, CELLS, CELLS), BF16),
                pltpu.VMEM((WIN_ROWS * WIN_COLS, LANES + 16, CELLS), BF16),
                pltpu.VMEM((2, CELLS, LANES), BF16),
                pltpu.VMEM((TILES, CHUNK, LANES), BF16),
                pltpu.SMEM((TILES,), I32),
                pltpu.SemaphoreType.DMA((4,)),
                pltpu.SemaphoreType.DMA,
                pltpu.SemaphoreType.DMA,
                pltpu.SemaphoreType.DMA((16,)),
                pltpu.SemaphoreType.DMA((SLOTS,)),
                pltpu.SemaphoreType.DMA((16,)),
                pltpu.SemaphoreType.DMA((16,)),
                pltpu.SemaphoreType.DMA((40,)),
                pltpu.SemaphoreType.DMA((WIN_ROWS, 8)),
                pltpu.SemaphoreType.DMA((WIN_ROWS,)),
                pltpu.SemaphoreType.DMA((WIN_ROWS,)),
                pltpu.SemaphoreType.DMA((16,)),
                pltpu.SemaphoreType.DMA((16,)),
            ],
            compiler_params=pltpu.CompilerParams(collective_id=0, has_side_effects=True),
        )(feats, weight, bias.reshape(1, LANES), neighbours, words, counts, tile_row)

    return jax.shard_map(
        per_device,
        mesh=mesh,
        in_specs=(
            P("tiles", "feat", None),
            P("feat", None),
            P(),
            P("tiles", None),
            P("tiles"),
            P("tiles", "feat", None, None),
            P(),
        ),
        out_specs=P("tiles", "feat", None),
        check_vma=False,
    )
```

```python
import functools

import jax
import jax.numpy as jnp
from jax import lax
from jax.experimental import pallas as pl
from jax.experimental.pallas import tpu as pltpu
from jax.sharding import PartitionSpec as P

MESH = pl.DeviceIdType.MESH
BF16 = jnp.bfloat16
F32 = jnp.float32
I32 = jnp.int32

SLOTS = 16
CELLS = 256
CHUNK = 16
WORDS = 24
BITS = 11
LANES = 128
TILES = 32
WIN_ROWS = 5
WIN_COLS = 6


def kernel(
    n_tiles,
    feats_hbm, weight_hbm, bias_ref, nb_hbm, words_hbm, counts_ref, rows_ref,
    out_ref,
    feats_v, words_v, weight_v, nb_own, nb_other, stage_f, stage_w, win, wbuf, wall, bits32, mask, feats_t, stage_o, obuf, inverse,
    local_sem, nb_send, nb_sem, word_send, word_sem, weight_send, weight_sem, win_send, win_sem, fwd_send, fwd_sem, out_send, out_sem,
):
    t = lax.axis_index("tiles")
    f = lax.axis_index("feat")
    z = t // 2
    core = t % 2
    partner = 2 * z + 1 - core
    row_in_plane = f // 2
    half = f % 2
    home = f // 8
    dest_row = 8 * z + row_in_plane
    n_planes = n_tiles // 2

    def device(tiles, feat):
        return {"tiles": tiles, "feat": feat}

    loads = [
        pltpu.make_async_copy(words_hbm, words_v, local_sem.at[0]),
        pltpu.make_async_copy(feats_hbm, feats_v, local_sem.at[1]),
        pltpu.make_async_copy(weight_hbm, weight_v, local_sem.at[2]),
        pltpu.make_async_copy(nb_hbm, nb_own, local_sem.at[3]),
    ]
    for load in loads:
        load.start()

    barrier = pltpu.get_barrier_semaphore()

    def greet(i, carry):
        tiles, feat = 2 * z + i // 16, i % 16

        @pl.when(jnp.logical_or(tiles != t, feat != f))
        def _():
            pl.semaphore_signal(barrier, inc=1, device_id=device(tiles, feat), device_id_type=MESH)

        return carry

    lax.fori_loop(0, 32, greet, 0)

    needs_before = jnp.logical_and(row_in_plane < 2, z > 0)
    needs_after = jnp.logical_and(row_in_plane >= 6, z < n_planes - 1)

    def greet_halo(tiles):
        def body(i, carry):
            pl.semaphore_signal(barrier, inc=1, device_id=device(tiles, core * 8 + i), device_id_type=MESH)
            return carry

        lax.fori_loop(0, 8, body, 0)

    @pl.when(needs_before)
    def _():
        greet_halo(2 * z - 1)

    @pl.when(needs_after)
    def _():
        greet_halo(2 * z + 2)

    for load in loads:
        load.wait()

    def order(s, carry):
        row = jnp.clip(rows_ref[t * TILES + s] - t * TILES, 0, TILES - 1)
        live = f < counts_ref[row]
        w = words_v[row]
        packed = w[:, :LANES] | (w[:, LANES:] << 16)
        stage_w[s] = jnp.where(live, packed, jnp.zeros_like(packed))
        stage_f[s // 8, s % 8] = feats_v[row]
        return carry

    lax.fori_loop(0, TILES, order, 0)

    sends_beyond = jnp.logical_or(
        jnp.logical_and(core == 1, z < n_planes - 1), jnp.logical_and(core == 0, z > 0)
    )

    @pl.when(sends_beyond)
    def _():
        pl.semaphore_wait(barrier, 35)

    @pl.when(jnp.logical_not(sends_beyond))
    def _():
        pl.semaphore_wait(barrier, 31)

    nb_copy = pltpu.make_async_remote_copy(
        nb_own, nb_other, nb_send, nb_sem, device_id=device(partner, f), device_id_type=MESH
    )
    nb_copy.start()

    def word_copy(i):
        chip = core * 8 + (i // 2 + f) % 8
        side = i % 2
        first = 4 * (chip % 8) + 2 * side
        mine = jnp.logical_and(chip == f, side == core)
        copy = pltpu.make_async_remote_copy(
            stage_w.at[pl.ds(first, 2)], wbuf.at[f], word_send.at[i], word_sem.at[f],
            device_id=device(2 * z + side, chip), device_id_type=MESH,
        )
        return copy, mine, first

    def start_words(i, carry):
        copy, mine, first = word_copy(i)

        @pl.when(jnp.logical_not(mine))
        def _():
            copy.start()

        @pl.when(mine)
        def _():
            wbuf[f] = stage_w[pl.ds(first, 2)]

        return carry

    lax.fori_loop(0, 16, start_words, 0)

    weight_mine = weight_v[...]
    wall[f] = weight_mine

    def weight_copy(i):
        chip = (f + i) % 16
        return pltpu.make_async_remote_copy(
            weight_v, wall.at[f], weight_send.at[i], weight_sem.at[f],
            device_id=device(t, chip), device_id_type=MESH,
        )

    def start_weight(i, carry):
        weight_copy(i).start()
        return carry

    lax.fori_loop(1, 16, start_weight, 0)

    my_cells = pl.ds(pl.multiple_of(f * CHUNK, CHUNK), CHUNK)

    feat_sends = []
    for i in range(40):
        step, h, r = i // 8 - 2, i // 4 % 2, i % 4
        to_row = 4 * t + r + step
        valid = jnp.logical_and(to_row >= 0, to_row < 4 * n_tiles)
        tiles = 2 * (to_row // 8) + home
        chip = 2 * (to_row % 8) + h
        sent = jnp.logical_and(valid, jnp.logical_or(tiles != t, chip != f))
        copy = pltpu.make_async_remote_copy(
            stage_f.at[r, pl.ds(2 * h, WIN_COLS)],
            win.at[2 - step, :, my_cells],
            win_send.at[i], win_sem.at[2 - step, f % 8],
            device_id=device(tiles, chip), device_id_type=MESH,
        )
        feat_sends.append((copy, sent))
        pl.when(sent)(copy.start)

    for r in range(4):
        w = 4 * t + r - dest_row + 2

        @pl.when(jnp.logical_and(home == core, jnp.logical_and(w >= 0, w < WIN_ROWS)))
        def _():
            win[w, :, my_cells] = stage_f[r, pl.ds(2 * half, WIN_COLS)]

    def invert(r, carry):
        found = 0
        for s in range(1, TILES):
            found = found + jnp.where(rows_ref[t * TILES + s] == t * TILES + r, s, 0)
        inverse[r] = jnp.clip(found, 0, TILES - 1)
        return carry

    lax.fori_loop(0, TILES, invert, 0)

    def row_exists(w):
        row = dest_row + w - 2
        return jnp.logical_and(row >= 0, row < 4 * n_tiles)

    def clear(w, carry):
        @pl.when(jnp.logical_not(row_exists(w)))
        def _():
            win[w] = jnp.zeros((WIN_COLS, CELLS, LANES), BF16)

        return carry

    lax.fori_loop(0, WIN_ROWS, clear, 0)

    ones_rows = jnp.ones((16, CELLS), BF16)

    def fill_ones(i, carry):
        feats_t[i, pl.ds(LANES, 16)] = ones_rows
        return carry

    lax.fori_loop(0, WIN_ROWS * WIN_COLS, fill_ones, 0)

    def unpack(k, carry):
        @pl.when(jnp.logical_not(jnp.logical_and(k == f, core == home)))
        def _():
            pltpu.make_async_copy(wbuf.at[k], wbuf.at[k], word_sem.at[k]).wait()

        for tile in range(2):
            packed = wbuf[k, tile]
            for b in range(BITS):
                bits32[0, pl.ds(b, WORDS, stride=BITS), :] = (packed >> b) & 1
                bits32[1, pl.ds(b, WORDS, stride=BITS), :] = (packed >> (16 + b)) & 1
            mask[tile, k, :, :LANES] = bits32[0, :CELLS].astype(F32).astype(BF16)
            mask[tile, k, :, LANES:] = bits32[1, :CELLS].astype(F32).astype(BF16)
        return carry

    lax.fori_loop(0, SLOTS, unpack, 0)

    kept = pl.ds(pl.multiple_of(core * LANES, LANES), LANES)

    def forward_copy(w):
        return pltpu.make_async_remote_copy(
            win.at[w, :, kept], win.at[w, :, kept], fwd_send.at[w], fwd_sem.at[w],
            device_id=device(partner, f), device_id_type=MESH,
        )

    def forward(w, carry):
        @pl.when(row_exists(w))
        def _():
            local = jnp.logical_and(home == core, (dest_row + w - 2) // 4 == t)

            def arrive(i, c):
                @pl.when(jnp.logical_not(jnp.logical_and(local, i == f % 8)))
                def _():
                    cells = pl.ds(pl.multiple_of((core * 8 + i) * CHUNK, CHUNK), CHUNK)
                    pltpu.make_async_copy(
                        win.at[w, :, cells], win.at[w, :, cells], win_sem.at[w, i]
                    ).wait()

                return c

            lax.fori_loop(0, 8, arrive, 0)
            forward_copy(w).start()

        return carry

    lax.fori_loop(0, WIN_ROWS, forward, 0)

    def turn(w, carry):
        @pl.when(row_exists(w))
        def _():
            forward_copy(w).wait_recv()

        for c in range(WIN_COLS):
            feats_t[w * WIN_COLS + c, pl.ds(0, LANES)] = win[w, c].T
        return carry

    lax.fori_loop(0, WIN_ROWS, turn, 0)

    nb_copy.wait_recv()

    def weight_wait(i, carry):
        chip = (f + i) % 16
        pltpu.make_async_copy(wall.at[chip], wall.at[chip], weight_sem.at[chip]).wait()
        return carry

    lax.fori_loop(1, 16, weight_wait, 0)
    weight = wall[...].astype(F32).reshape(LANES, LANES).astype(BF16)
    bias = bias_ref[...]
    band = 2 * z + home

    firsts = 4 * (f % 8) + 2 * core
    rows = [
        jnp.clip(rows_ref[band * TILES + firsts + tile] - band * TILES, 0, TILES - 1) for tile in range(2)
    ]

    def add(k, totals):
        done = []
        for tile in range(2):
            near = jnp.where(home == core, nb_own[k, rows[tile]], nb_other[k, rows[tile]])
            place = (near // 8 - (dest_row - 2)) * WIN_COLS + near % 8 - 2 * half
            place = jnp.clip(place, 0, WIN_ROWS * WIN_COLS - 1)
            done.append(totals[tile] + jnp.dot(feats_t[place], mask[tile, k], preferred_element_type=F32))
        return tuple(done)

    zero = jnp.zeros((LANES + 16, CELLS), F32)
    totals = lax.fori_loop(0, SLOTS, add, (zero, zero), unroll=True)
    for tile in range(2):
        total = totals[tile].T
        base = win[2, 4 * half + 2 * core + tile - 2 * half].astype(F32)
        degree = total[:, LANES : LANES + 1]
        normed = ((total[:, :LANES] + base) / jnp.sqrt(degree + 1.0)).astype(BF16)
        linear = jnp.dot(normed, weight, preferred_element_type=F32) + bias
        stage_o[tile] = (base + jnp.maximum(linear, 0.0)).astype(BF16)

    first_out = 4 * (f % 8) + 2 * core

    def out_copy(i):
        chip = (f + i) % 16
        cells = pl.ds(pl.multiple_of(chip * CHUNK, CHUNK), CHUNK)
        mine = jnp.logical_and(i == 0, home == core)
        copy = pltpu.make_async_remote_copy(
            stage_o.at[:, cells], obuf.at[pl.ds(first_out, 2)], out_send.at[i], out_sem.at[first_out // 2],
            device_id=device(2 * z + home, chip), device_id_type=MESH,
        )
        return copy, mine

    def start_out(i, carry):
        copy, mine = out_copy(i)

        @pl.when(jnp.logical_not(mine))
        def _():
            copy.start()

        @pl.when(mine)
        def _():
            obuf[pl.ds(first_out, 2)] = stage_o[:, my_cells]

        return carry

    lax.fori_loop(0, 16, start_out, 0)

    nb_copy.wait_send()

    def end_words(i, carry):
        copy, mine, _ = word_copy(i)

        @pl.when(jnp.logical_not(mine))
        def _():
            copy.wait_send()

        return carry

    lax.fori_loop(0, 16, end_words, 0)

    def end_weight(i, carry):
        weight_copy(i).wait_send()
        return carry

    lax.fori_loop(1, 16, end_weight, 0)

    for copy, sent in feat_sends:
        pl.when(sent)(copy.wait_send)

    def end_forward(w, carry):
        @pl.when(row_exists(w))
        def _():
            forward_copy(w).wait_send()

        return carry

    lax.fori_loop(0, WIN_ROWS, end_forward, 0)

    def end_out(i, carry):
        copy, mine = out_copy(i)

        @pl.when(jnp.logical_not(mine))
        def _():
            copy.wait_send()

        return carry

    lax.fori_loop(0, 16, end_out, 0)

    def arrive_out(i, carry):
        @pl.when(jnp.logical_not(jnp.logical_and(home == core, i == first_out // 2)))
        def _():
            pair = pl.ds(2 * i, 2)
            pltpu.make_async_copy(obuf.at[pair], obuf.at[pair], out_sem.at[i]).wait()

        return carry

    lax.fori_loop(0, 16, arrive_out, 0)

    def put(r, carry):
        out_ref[r] = obuf[inverse[r]]
        return carry

    lax.fori_loop(0, TILES, put, 0)


def solution(mesh):
    n_tiles = mesh.shape["tiles"]

    def per_device(feats, weight, bias, neighbours, counts, adj_words, tile_row):
        vmem = pl.BlockSpec(memory_space=pltpu.VMEM)
        smem = pl.BlockSpec(memory_space=pltpu.SMEM)
        hbm = pl.BlockSpec(memory_space=pl.ANY)
        words = adj_words.reshape(TILES, WORDS, CELLS)
        return pl.pallas_call(
            functools.partial(kernel, n_tiles),
            out_shape=jax.ShapeDtypeStruct(feats.shape, BF16),
            in_specs=[hbm, hbm, vmem, hbm, hbm, smem, smem],
            out_specs=vmem,
            scratch_shapes=[
                pltpu.VMEM((TILES, CHUNK, LANES), BF16),
                pltpu.VMEM((TILES, WORDS, CELLS), I32),
                pltpu.VMEM((8, LANES), BF16),
                pltpu.SMEM((SLOTS, TILES), I32),
                pltpu.SMEM((SLOTS, TILES), I32),
                pltpu.VMEM((4, 8, CHUNK, LANES), BF16),
                pltpu.VMEM((TILES, WORDS, LANES), I32),
                pltpu.VMEM((WIN_ROWS, WIN_COLS, CELLS, LANES), BF16),
                pltpu.VMEM((SLOTS, 2, WORDS, LANES), I32),
                pltpu.VMEM((16, 8, LANES), BF16),
                pltpu.VMEM((2, WORDS * BITS, LANES), I32),
                pltpu.VMEM((2, SLOTS, CELLS, CELLS), BF16),
                pltpu.VMEM((WIN_ROWS * WIN_COLS, LANES + 16, CELLS), BF16),
                pltpu.VMEM((2, CELLS, LANES), BF16),
                pltpu.VMEM((TILES, CHUNK, LANES), BF16),
                pltpu.SMEM((TILES,), I32),
                pltpu.SemaphoreType.DMA((4,)),
                pltpu.SemaphoreType.DMA,
                pltpu.SemaphoreType.DMA,
                pltpu.SemaphoreType.DMA((16,)),
                pltpu.SemaphoreType.DMA((SLOTS,)),
                pltpu.SemaphoreType.DMA((16,)),
                pltpu.SemaphoreType.DMA((16,)),
                pltpu.SemaphoreType.DMA((40,)),
                pltpu.SemaphoreType.DMA((WIN_ROWS, 8)),
                pltpu.SemaphoreType.DMA((WIN_ROWS,)),
                pltpu.SemaphoreType.DMA((WIN_ROWS,)),
                pltpu.SemaphoreType.DMA((16,)),
                pltpu.SemaphoreType.DMA((16,)),
            ],
            compiler_params=pltpu.CompilerParams(collective_id=0, has_side_effects=True),
        )(feats, weight, bias.reshape(1, LANES), neighbours.T, words, counts, tile_row)

    return jax.shard_map(
        per_device,
        mesh=mesh,
        in_specs=(
            P("tiles", "feat", None),
            P("feat", None),
            P(),
            P("tiles", None),
            P("tiles"),
            P("tiles", "feat", None, None),
            P(),
        ),
        out_specs=P("tiles", "feat", None),
        check_vma=False,
    )
```

```python
import functools

import jax
import jax.numpy as jnp
from jax import lax
from jax.experimental import pallas as pl
from jax.experimental.pallas import tpu as pltpu
from jax.sharding import PartitionSpec as P

MESH = pl.DeviceIdType.MESH
STEPS = (
    (2, 2), (1, 2), (3, 2), (2, 1), (2, 3), (0, 2), (2, 0), (1, 1),
    (3, 3), (1, 3), (3, 1), (0, 1), (0, 3), (1, 0), (3, 0), (0, 0),
)
BF16 = jnp.bfloat16
F32 = jnp.float32
I32 = jnp.int32

SLOTS = 16
CELLS = 256
CHUNK = 16
WORDS = 24
BITS = 11
LANES = 128
TILES = 32
WIN_ROWS = 5
WIN_COLS = 6


def kernel(
    n_tiles,
    feats_hbm, weight_hbm, bias_hbm, nb_hbm, words_hbm, counts_hbm, rows_hbm,
    out_ref,
    feats_v, words_v, weight_v, bias_ref, counts_ref, rows_ref, nb_own, nb_other, stage_f, stage_w, win, wbuf, wall, bits32, mask, feats_t, stage_o, obuf, inverse,
    local_sem, nb_send, nb_sem, word_send, word_sem, weight_send, weight_sem, win_send, win_sem, fwd_send, fwd_sem, out_send, out_sem,
):
    t = lax.axis_index("tiles")
    f = lax.axis_index("feat")
    z = t // 2
    core = t % 2
    partner = 2 * z + 1 - core
    row_in_plane = f // 2
    half = f % 2
    home = f // 8
    dest_row = 8 * z + row_in_plane
    n_planes = n_tiles // 2

    def device(tiles, feat):
        return {"tiles": tiles, "feat": feat}

    loads = [
        pltpu.make_async_copy(words_hbm, words_v, local_sem.at[0]),
        pltpu.make_async_copy(feats_hbm, feats_v, local_sem.at[1]),
        pltpu.make_async_copy(weight_hbm, weight_v, local_sem.at[2]),
        pltpu.make_async_copy(nb_hbm, nb_own, local_sem.at[3]),
        pltpu.make_async_copy(bias_hbm, bias_ref, local_sem.at[4]),
        pltpu.make_async_copy(counts_hbm, counts_ref, local_sem.at[5]),
        pltpu.make_async_copy(rows_hbm, rows_ref, local_sem.at[6]),
    ]
    for load in loads:
        load.start()

    barrier = pltpu.get_barrier_semaphore()

    chips = [(f // 4 + dy) % 4 * 4 + (f % 4 + dx) % 4 for dy, dx in STEPS]

    for i, chip in enumerate(chips):
        for tiles in (partner,) if STEPS[i] == (0, 0) else (t, partner):
            pl.semaphore_signal(barrier, inc=1, device_id=device(tiles, chip), device_id_type=MESH)

    needs_before = jnp.logical_and(row_in_plane < 2, z > 0)
    needs_after = jnp.logical_and(row_in_plane >= 6, z < n_planes - 1)

    def greet_halo(tiles):
        def body(i, carry):
            pl.semaphore_signal(barrier, inc=1, device_id=device(tiles, core * 8 + i), device_id_type=MESH)
            return carry

        lax.fori_loop(0, 8, body, 0)

    @pl.when(needs_before)
    def _():
        greet_halo(2 * z - 1)

    @pl.when(needs_after)
    def _():
        greet_halo(2 * z + 2)

    for load in loads:
        load.wait()

    def order(s, carry):
        row = jnp.clip(rows_ref[t * TILES + s] - t * TILES, 0, TILES - 1)
        live = f < counts_ref[row]
        w = words_v[row]
        packed = w[:, :LANES] | (w[:, LANES:] << 16)
        stage_w[s] = jnp.where(live, packed, jnp.zeros_like(packed))
        stage_f[s // 8, s % 8] = feats_v[row]
        return carry

    lax.fori_loop(0, TILES, order, 0)

    sends_beyond = jnp.logical_or(
        jnp.logical_and(core == 1, z < n_planes - 1), jnp.logical_and(core == 0, z > 0)
    )

    @pl.when(sends_beyond)
    def _():
        pl.semaphore_wait(barrier, 35)

    @pl.when(jnp.logical_not(sends_beyond))
    def _():
        pl.semaphore_wait(barrier, 31)

    nb_copy = pltpu.make_async_remote_copy(
        nb_own, nb_other, nb_send, nb_sem, device_id=device(partner, f), device_id_type=MESH
    )
    nb_copy.start()

    word_sends = []
    for i, chip in enumerate(chips):
        for side in range(2):
            sent = chip // 8 == core
            if STEPS[i] == (0, 0):
                sent = jnp.logical_and(sent, side != core)
            copy = pltpu.make_async_remote_copy(
                stage_w.at[pl.ds(4 * (chip % 8) + 2 * side, 2)], wbuf.at[f],
                word_send.at[2 * i + side], word_sem.at[f],
                device_id=device(2 * z + side, chip), device_id_type=MESH,
            )
            word_sends.append((copy, sent))
            pl.when(sent)(copy.start)

    @pl.when(home == core)
    def _():
        wbuf[f] = stage_w[pl.ds(4 * (f % 8) + 2 * core, 2)]

    weight_mine = weight_v[...]
    wall[f] = weight_mine

    def weight_copy(i):
        chip = (f + i) % 16
        return pltpu.make_async_remote_copy(
            weight_v, wall.at[f], weight_send.at[i], weight_sem.at[f],
            device_id=device(t, chip), device_id_type=MESH,
        )

    def start_weight(i, carry):
        weight_copy(i).start()
        return carry

    lax.fori_loop(1, 16, start_weight, 0)

    my_cells = pl.ds(pl.multiple_of(f * CHUNK, CHUNK), CHUNK)

    feat_sends = []
    for i, chip in enumerate(chips):
        ahead = jnp.where(core == 0, (chip // 2 + 2) % 8 - 2, (chip // 2 + 6) % 8 - 2)
        to_row = 4 * t + ahead
        inside = jnp.logical_and(to_row >= 0, to_row < 4 * n_tiles)
        tiles = 2 * (to_row // 8) + home
        for r in range(4):
            sent = jnp.logical_and(inside, jnp.logical_and(ahead - r >= -2, ahead - r <= 2))
            if STEPS[i] == (0, 0):
                sent = jnp.logical_and(sent, tiles != t)
            w = jnp.clip(r - ahead + 2, 0, WIN_ROWS - 1)
            copy = pltpu.make_async_remote_copy(
                stage_f.at[r, pl.ds(2 * (chip % 2), WIN_COLS)],
                win.at[w, :, my_cells],
                win_send.at[4 * i + r], win_sem.at[w, f % 8],
                device_id=device(tiles, chip), device_id_type=MESH,
            )
            feat_sends.append((copy, sent))
            pl.when(sent)(copy.start)

    for r in range(4):
        w = 4 * t + r - dest_row + 2

        @pl.when(jnp.logical_and(home == core, jnp.logical_and(w >= 0, w < WIN_ROWS)))
        def _():
            win[w, :, my_cells] = stage_f[r, pl.ds(2 * half, WIN_COLS)]

    def invert(r, carry):
        found = 0
        for s in range(1, TILES):
            found = found + jnp.where(rows_ref[t * TILES + s] == t * TILES + r, s, 0)
        inverse[r] = jnp.clip(found, 0, TILES - 1)
        return carry

    lax.fori_loop(0, TILES, invert, 0)

    def row_exists(w):
        row = dest_row + w - 2
        return jnp.logical_and(row >= 0, row < 4 * n_tiles)

    def clear(w, carry):
        @pl.when(jnp.logical_not(row_exists(w)))
        def _():
            win[w] = jnp.zeros((WIN_COLS, CELLS, LANES), BF16)

        return carry

    lax.fori_loop(0, WIN_ROWS, clear, 0)

    ones_rows = jnp.ones((16, LANES), BF16)

    def fill_ones(i, carry):
        feats_t[0, i, pl.ds(LANES, 16)] = ones_rows
        feats_t[1, i, pl.ds(LANES, 16)] = ones_rows
        return carry

    lax.fori_loop(0, WIN_ROWS * WIN_COLS, fill_ones, 0)

    def unpack(k, carry):
        @pl.when(jnp.logical_not(jnp.logical_and(k == f, core == home)))
        def _():
            pltpu.make_async_copy(wbuf.at[k], wbuf.at[k], word_sem.at[k]).wait()

        for tile in range(2):
            packed = wbuf[k, tile]
            for b in range(BITS):
                bits32[0, pl.ds(b, WORDS, stride=BITS), :] = (packed >> b) & 1
                bits32[1, pl.ds(b, WORDS, stride=BITS), :] = (packed >> (16 + b)) & 1
            mask[tile, k, :, :LANES] = bits32[0, :CELLS].astype(F32).astype(BF16)
            mask[tile, k, :, LANES:] = bits32[1, :CELLS].astype(F32).astype(BF16)
        return carry

    lax.fori_loop(0, SLOTS, unpack, 0)

    nb_copy.wait_recv()

    def weight_wait(i, carry):
        chip = (f + i) % 16
        pltpu.make_async_copy(wall.at[chip], wall.at[chip], weight_sem.at[chip]).wait()
        return carry

    lax.fori_loop(1, 16, weight_wait, 0)
    kept = pl.ds(pl.multiple_of(core * LANES, LANES), LANES)

    def forward_copy(w):
        return pltpu.make_async_remote_copy(
            win.at[w, :, kept], win.at[w, :, kept], fwd_send.at[w], fwd_sem.at[w],
            device_id=device(partner, f), device_id_type=MESH,
        )

    def forward(w, carry):
        @pl.when(row_exists(w))
        def _():
            local = jnp.logical_and(home == core, (dest_row + w - 2) // 4 == t)

            def arrive(i, c):
                @pl.when(jnp.logical_not(jnp.logical_and(local, i == f % 8)))
                def _():
                    cells = pl.ds(pl.multiple_of((core * 8 + i) * CHUNK, CHUNK), CHUNK)
                    pltpu.make_async_copy(
                        win.at[w, :, cells], win.at[w, :, cells], win_sem.at[w, i]
                    ).wait()

                return c

            lax.fori_loop(0, 8, arrive, 0)
            forward_copy(w).start()

        return carry

    lax.fori_loop(0, WIN_ROWS, forward, 0)

    given = pl.ds(pl.multiple_of((1 - core) * LANES, LANES), LANES)

    def turn_kept(w, carry):
        for c in range(WIN_COLS):
            feats_t[core, w * WIN_COLS + c, pl.ds(0, LANES)] = win[w, c, kept].T
        return carry

    lax.fori_loop(0, WIN_ROWS, turn_kept, 0)

    def turn_given(w, carry):
        @pl.when(row_exists(w))
        def _():
            forward_copy(w).wait_recv()

        for c in range(WIN_COLS):
            feats_t[1 - core, w * WIN_COLS + c, pl.ds(0, LANES)] = win[w, c, given].T
        return carry

    lax.fori_loop(0, WIN_ROWS, turn_given, 0)

    weight = wall[...].astype(F32).reshape(LANES, LANES).astype(BF16)
    bias = bias_ref[...]
    band = 2 * z + home

    firsts = 4 * (f % 8) + 2 * core
    rows = [
        jnp.clip(rows_ref[band * TILES + firsts + tile] - band * TILES, 0, TILES - 1) for tile in range(2)
    ]

    def add(k, totals):
        done = []
        for tile in range(2):
            near = jnp.where(home == core, nb_own[k, rows[tile]], nb_other[k, rows[tile]])
            place = (near // 8 - (dest_row - 2)) * WIN_COLS + near % 8 - 2 * half
            place = jnp.clip(place, 0, WIN_ROWS * WIN_COLS - 1)
            done.append(totals[tile] + jnp.dot(
                jnp.concatenate([feats_t[0, place], feats_t[1, place]], axis=1), mask[tile, k],
                preferred_element_type=F32,
            ))
        return tuple(done)

    zero = jnp.zeros((LANES + 16, CELLS), F32)
    totals = lax.fori_loop(0, SLOTS, add, (zero, zero), unroll=True)
    for tile in range(2):
        total = totals[tile].T
        base = win[2, 4 * half + 2 * core + tile - 2 * half].astype(F32)
        degree = total[:, LANES : LANES + 1]
        normed = ((total[:, :LANES] + base) / jnp.sqrt(degree + 1.0)).astype(BF16)
        linear = jnp.dot(normed, weight, preferred_element_type=F32) + bias
        stage_o[tile] = (base + jnp.maximum(linear, 0.0)).astype(BF16)

    first_out = 4 * (f % 8) + 2 * core

    out_sends = []
    for i, chip in enumerate(chips):
        cells = pl.ds(pl.multiple_of(chip * CHUNK, CHUNK), CHUNK)
        copy = pltpu.make_async_remote_copy(
            stage_o.at[:, cells], obuf.at[pl.ds(first_out, 2)],
            out_send.at[i], out_sem.at[first_out // 2],
            device_id=device(2 * z + home, chip), device_id_type=MESH,
        )
        sent = home != core if STEPS[i] == (0, 0) else True
        out_sends.append((copy, sent))
        if sent is True:
            copy.start()
        else:
            pl.when(sent)(copy.start)

    @pl.when(home == core)
    def _():
        obuf[pl.ds(first_out, 2)] = stage_o[:, my_cells]

    nb_copy.wait_send()

    for copy, sent in word_sends:
        pl.when(sent)(copy.wait_send)

    def end_weight(i, carry):
        weight_copy(i).wait_send()
        return carry

    lax.fori_loop(1, 16, end_weight, 0)

    for copy, sent in feat_sends:
        pl.when(sent)(copy.wait_send)

    def end_forward(w, carry):
        @pl.when(row_exists(w))
        def _():
            forward_copy(w).wait_send()

        return carry

    lax.fori_loop(0, WIN_ROWS, end_forward, 0)

    for copy, sent in out_sends:
        if sent is True:
            copy.wait_send()
        else:
            pl.when(sent)(copy.wait_send)

    def arrive_out(i, carry):
        @pl.when(jnp.logical_not(jnp.logical_and(home == core, i == first_out // 2)))
        def _():
            pair = pl.ds(2 * i, 2)
            pltpu.make_async_copy(obuf.at[pair], obuf.at[pair], out_sem.at[i]).wait()

        return carry

    lax.fori_loop(0, 16, arrive_out, 0)

    def put(r, carry):
        out_ref[r] = obuf[inverse[r]]
        return carry

    lax.fori_loop(0, TILES, put, 0)


def solution(mesh):
    n_tiles = mesh.shape["tiles"]

    def per_device(feats, weight, bias, neighbours, counts, adj_words, tile_row):
        vmem = pl.BlockSpec(memory_space=pltpu.VMEM)
        hbm = pl.BlockSpec(memory_space=pl.ANY)
        words = adj_words.reshape(TILES, WORDS, CELLS)
        return pl.pallas_call(
            functools.partial(kernel, n_tiles),
            out_shape=pltpu.VMEM(feats.shape, BF16),
            in_specs=[hbm] * 7,
            out_specs=vmem,
            scratch_shapes=[
                pltpu.VMEM((TILES, CHUNK, LANES), BF16),
                pltpu.VMEM((TILES, WORDS, CELLS), I32),
                pltpu.VMEM((8, LANES), BF16),
                pltpu.VMEM((1, LANES), F32),
                pltpu.SMEM((TILES,), I32),
                pltpu.SMEM((n_tiles * TILES,), I32),
                pltpu.SMEM((SLOTS, TILES), I32),
                pltpu.SMEM((SLOTS, TILES), I32),
                pltpu.VMEM((4, 8, CHUNK, LANES), BF16),
                pltpu.VMEM((TILES, WORDS, LANES), I32),
                pltpu.VMEM((WIN_ROWS, WIN_COLS, CELLS, LANES), BF16),
                pltpu.VMEM((SLOTS, 2, WORDS, LANES), I32),
                pltpu.VMEM((16, 8, LANES), BF16),
                pltpu.VMEM((2, WORDS * BITS, LANES), I32),
                pltpu.VMEM((2, SLOTS, CELLS, CELLS), BF16),
                pltpu.VMEM((2, WIN_ROWS * WIN_COLS, LANES + 16, LANES), BF16),
                pltpu.VMEM((2, CELLS, LANES), BF16),
                pltpu.VMEM((TILES, CHUNK, LANES), BF16),
                pltpu.SMEM((TILES,), I32),
                pltpu.SemaphoreType.DMA((7,)),
                pltpu.SemaphoreType.DMA,
                pltpu.SemaphoreType.DMA,
                pltpu.SemaphoreType.DMA((32,)),
                pltpu.SemaphoreType.DMA((SLOTS,)),
                pltpu.SemaphoreType.DMA((16,)),
                pltpu.SemaphoreType.DMA((16,)),
                pltpu.SemaphoreType.DMA((64,)),
                pltpu.SemaphoreType.DMA((WIN_ROWS, 8)),
                pltpu.SemaphoreType.DMA((WIN_ROWS,)),
                pltpu.SemaphoreType.DMA((WIN_ROWS,)),
                pltpu.SemaphoreType.DMA((16,)),
                pltpu.SemaphoreType.DMA((16,)),
            ],
            compiler_params=pltpu.CompilerParams(collective_id=0, has_side_effects=True),
        )(feats, weight, bias.reshape(1, LANES), neighbours.T, words, counts, tile_row)

    return jax.shard_map(
        per_device,
        mesh=mesh,
        in_specs=(
            P("tiles", "feat", None),
            P("feat", None),
            P(),
            P("tiles", None),
            P("tiles"),
            P("tiles", "feat", None, None),
            P(),
        ),
        out_specs=P("tiles", "feat", None),
        check_vma=False,
    )
```

```python
import functools

import jax
import jax.numpy as jnp
from jax import lax
from jax.experimental import pallas as pl
from jax.experimental.pallas import tpu as pltpu
from jax.sharding import PartitionSpec as P

MESH = pl.DeviceIdType.MESH
STEPS = (
    (2, 2), (1, 2), (3, 2), (2, 1), (2, 3), (0, 2), (2, 0), (1, 1),
    (3, 3), (1, 3), (3, 1), (0, 1), (0, 3), (1, 0), (3, 0), (0, 0),
)
BF16 = jnp.bfloat16
F32 = jnp.float32
I32 = jnp.int32

SLOTS = 16
CELLS = 256
CHUNK = 16
WORDS = 24
BITS = 11
LANES = 128
TILES = 32
WIN_ROWS = 5
WIN_COLS = 6


def kernel(
    n_tiles,
    feats_hbm, weight_hbm, bias_hbm, nb_hbm, words_hbm, counts_hbm, rows_hbm,
    out_ref,
    feats_v, words_v, weight_v, bias_ref, counts_ref, rows_ref, nb_own, nb_other, stage_f, stage_w, relay_y, relay_x, win, wbuf, wall, bits32, mask, feats_t, stage_o, obuf, inverse,
    local_sem, nb_send, nb_sem, word_send, word_sem, weight_send, weight_sem, to_y_send, to_y_sem, to_x_send, to_x_sem, win_y_send, win_y_sem, win_x_send, win_x_sem, fwd_send, fwd_sem, out_send, out_sem,
):
    t = lax.axis_index("tiles")
    f = lax.axis_index("feat")
    z = t // 2
    core = t % 2
    partner = 2 * z + 1 - core
    row_in_plane = f // 2
    y, x = f // 4, f % 4
    half = f % 2
    home = f // 8
    dest_row = 8 * z + row_in_plane
    n_planes = n_tiles // 2

    def device(tiles, feat):
        return {"tiles": tiles, "feat": feat}

    loads = [
        pltpu.make_async_copy(words_hbm, words_v, local_sem.at[0]),
        pltpu.make_async_copy(feats_hbm, feats_v, local_sem.at[1]),
        pltpu.make_async_copy(weight_hbm, weight_v, local_sem.at[2]),
        pltpu.make_async_copy(nb_hbm, nb_own, local_sem.at[3]),
        pltpu.make_async_copy(bias_hbm, bias_ref, local_sem.at[4]),
        pltpu.make_async_copy(counts_hbm, counts_ref, local_sem.at[5]),
        pltpu.make_async_copy(rows_hbm, rows_ref, local_sem.at[6]),
    ]
    for load in loads:
        load.start()

    barrier = pltpu.get_barrier_semaphore()

    chips = [(f // 4 + dy) % 4 * 4 + (f % 4 + dx) % 4 for dy, dx in STEPS]

    for i, chip in enumerate(chips):
        for tiles in (partner,) if STEPS[i] == (0, 0) else (t, partner):
            pl.semaphore_signal(barrier, inc=1, device_id=device(tiles, chip), device_id_type=MESH)

    def plane_for(chip_y):
        below = jnp.logical_and(core == 0, chip_y == 3).astype(I32)
        above = jnp.logical_and(core == 1, chip_y == 0).astype(I32)
        return z - below + above

    def ahead_of(chip_y):
        return (2 * chip_y + jnp.where(core == 0, 2, 6)) % 8 - 2

    def in_slide(plane):
        return jnp.logical_and(plane >= 0, plane < n_planes)

    for source_y in range(4):
        above = jnp.logical_and(y == 3, z < n_planes - 1)
        below = jnp.logical_and(y == 0, z > 0)
        if source_y < 2:
            above = jnp.logical_and(above, core == 0)
        else:
            below = jnp.logical_and(below, core == 1)

        @pl.when(above)
        def _():
            pl.semaphore_signal(
                barrier, inc=1, device_id=device(2 * z + 2, 4 * source_y + x), device_id_type=MESH
            )

        @pl.when(below)
        def _():
            pl.semaphore_signal(
                barrier, inc=1, device_id=device(2 * z - 1, 4 * source_y + x), device_id_type=MESH
            )

    for load in loads:
        load.wait()

    def order(s, carry):
        row = jnp.clip(rows_ref[t * TILES + s] - t * TILES, 0, TILES - 1)
        live = f < counts_ref[row]
        w = words_v[row]
        packed = w[:, :LANES] | (w[:, LANES:] << 16)
        stage_w[s] = jnp.where(live, packed, jnp.zeros_like(packed))
        stage_f[s // 8, s % 8] = feats_v[row]
        return carry

    lax.fori_loop(0, TILES, order, 0)

    beyond = jnp.where(
        core == 0, jnp.where(z > 0, 1 + y // 2, 0), jnp.where(z < n_planes - 1, 2 - y // 2, 0)
    )
    for peers in range(3):

        @pl.when(beyond == peers)
        def _():
            pl.semaphore_wait(barrier, 31 + peers)

    first_sends = []

    def reaches(r, ahead):
        return jnp.logical_and(ahead >= r - 3, ahead <= r + 2)

    def send(copy, sent, sends):
        sends.append((copy, sent))
        if sent is True:
            copy.start()
        else:
            pl.when(sent)(copy.start)

    for step in (2, 1, 3, 0):
        to_y = (y + step) % 4
        plane = plane_for(to_y)
        for i in range(2):
            sent = jnp.logical_and(in_slide(plane), reaches(2 * i, ahead_of(to_y)))
            if step == 0:
                mine = jnp.logical_and(sent, plane == z)
                sent = jnp.logical_and(sent, plane != z)

                @pl.when(mine)
                def _():
                    relay_y[i, :, y] = stage_f[2 * i]

            copy = pltpu.make_async_remote_copy(
                stage_f.at[2 * i], relay_y.at[i, :, y], to_y_send.at[i, step], to_y_sem.at[i, y],
                device_id=device(2 * plane + core, 4 * to_y + x), device_id_type=MESH,
            )
            send(copy, sent, first_sends)
        to_x = (x + step) % 4
        for i in range(2):
            columns = pl.ds(2 * (to_x % 2), WIN_COLS)
            if step == 0:
                relay_x[i, :, x] = stage_f[2 * i + 1, columns]
            else:
                copy = pltpu.make_async_remote_copy(
                    stage_f.at[2 * i + 1, columns], relay_x.at[i, :, x],
                    to_x_send.at[i, step], to_x_sem.at[i, x],
                    device_id=device(t, 4 * y + to_x), device_id_type=MESH,
                )
                send(copy, True, first_sends)

    nb_copy = pltpu.make_async_remote_copy(
        nb_own, nb_other, nb_send, nb_sem, device_id=device(partner, f), device_id_type=MESH
    )
    nb_copy.start()

    word_sends = []
    for i, chip in enumerate(chips):
        for side in range(2):
            sent = chip // 8 == core
            if STEPS[i] == (0, 0):
                sent = jnp.logical_and(sent, side != core)
            copy = pltpu.make_async_remote_copy(
                stage_w.at[pl.ds(4 * (chip % 8) + 2 * side, 2)], wbuf.at[f],
                word_send.at[2 * i + side], word_sem.at[f],
                device_id=device(2 * z + side, chip), device_id_type=MESH,
            )
            word_sends.append((copy, sent))
            pl.when(sent)(copy.start)

    @pl.when(home == core)
    def _():
        wbuf[f] = stage_w[pl.ds(4 * (f % 8) + 2 * core, 2)]

    weight_mine = weight_v[...]
    wall[f] = weight_mine

    def weight_copy(i):
        chip = (f + i) % 16
        return pltpu.make_async_remote_copy(
            weight_v, wall.at[f], weight_send.at[i], weight_sem.at[f],
            device_id=device(t, chip), device_id_type=MESH,
        )

    def start_weight(i, carry):
        weight_copy(i).start()
        return carry

    lax.fori_loop(1, 16, start_weight, 0)

    def row_exists(w):
        row = dest_row + w - 2
        return jnp.logical_and(row >= 0, row < 4 * n_tiles)

    def clear(w, carry):
        @pl.when(jnp.logical_not(row_exists(w)))
        def _():
            win[w] = jnp.zeros((WIN_COLS, 4, 4, CHUNK, LANES), BF16)

        return carry

    lax.fori_loop(0, WIN_ROWS, clear, 0)

    ones_rows = jnp.ones((16, LANES), BF16)

    def fill_ones(i, carry):
        feats_t[0, i, pl.ds(LANES, 16)] = ones_rows
        feats_t[1, i, pl.ds(LANES, 16)] = ones_rows
        return carry

    lax.fori_loop(0, WIN_ROWS * WIN_COLS, fill_ones, 0)

    my_cells = pl.ds(pl.multiple_of(f * CHUNK, CHUNK), CHUNK)
    second_sends = []
    ahead = ahead_of(y)
    band_plane = z + jnp.logical_and(core == 0, y == 3).astype(I32) - jnp.logical_and(
        core == 1, y == 0).astype(I32)

    for i in range(2):
        r = 2 * i
        here = jnp.logical_and(in_slide(band_plane), reaches(r, ahead))
        for source_y in range(4):

            @pl.when(jnp.logical_and(here, jnp.logical_or(band_plane != z, y != source_y)))
            def _():
                pltpu.make_async_copy(
                    relay_y.at[i, :, source_y], relay_y.at[i, :, source_y], to_y_sem.at[i, source_y]
                ).wait()

        for step in (2, 1, 3, 0):
            to_x = (x + step) % 4
            gap = ahead + to_x // 2 - r
            w = jnp.clip(2 - gap, 0, WIN_ROWS - 1)
            columns = pl.ds(2 * (to_x % 2), WIN_COLS)
            needed = jnp.logical_and(here, jnp.logical_and(gap >= -2, gap <= 2))
            for q in range(2):
                sent = needed
                if step == 0:
                    sent = jnp.logical_and(needed, core != q)

                    @pl.when(jnp.logical_and(needed, core == q))
                    def _():
                        win[w, :, 2 * q : 2 * q + 2, x] = relay_y[i, columns, 2 * q : 2 * q + 2]

                copy = pltpu.make_async_remote_copy(
                    relay_y.at[i, columns, pl.ds(2 * q, 2)], win.at[w, :, pl.ds(2 * q, 2), x],
                    win_y_send.at[i, step, q], win_y_sem.at[w, x],
                    device_id=device(2 * z + q, 4 * y + to_x), device_id_type=MESH,
                )
                send(copy, sent, second_sends)

        r = 2 * i + 1
        for step in range(1, 4):
            source_x = (x + step) % 4
            pltpu.make_async_copy(
                relay_x.at[i, :, source_x], relay_x.at[i, :, source_x], to_x_sem.at[i, source_x]
            ).wait()

        for step in (2, 1, 3, 0):
            to_y = (y + step) % 4
            plane = plane_for(to_y)
            gap = ahead_of(to_y) + x // 2 - r
            w = jnp.clip(2 - gap, 0, WIN_ROWS - 1)
            sent = jnp.logical_and(in_slide(plane), jnp.logical_and(gap >= -2, gap <= 2))
            if step == 0:
                at_home = jnp.logical_and(plane == z, home == core)
                mine = jnp.logical_and(sent, at_home)
                sent = jnp.logical_and(sent, jnp.logical_not(at_home))

                @pl.when(mine)
                def _():
                    win[w, :, y] = relay_x[i]

            copy = pltpu.make_async_remote_copy(
                relay_x.at[i], win.at[w, :, y], win_x_send.at[i, step], win_x_sem.at[w, y % 2],
                device_id=device(2 * plane + home, 4 * to_y + x), device_id_type=MESH,
            )
            send(copy, sent, second_sends)

    def invert(r, carry):
        found = 0
        for s in range(1, TILES):
            found = found + jnp.where(rows_ref[t * TILES + s] == t * TILES + r, s, 0)
        inverse[r] = jnp.clip(found, 0, TILES - 1)
        return carry

    lax.fori_loop(0, TILES, invert, 0)

    def unpack(k, carry):
        @pl.when(jnp.logical_not(jnp.logical_and(k == f, core == home)))
        def _():
            pltpu.make_async_copy(wbuf.at[k], wbuf.at[k], word_sem.at[k]).wait()

        for tile in range(2):
            packed = wbuf[k, tile]
            for b in range(BITS):
                bits32[0, pl.ds(b, WORDS, stride=BITS), :] = (packed >> b) & 1
                bits32[1, pl.ds(b, WORDS, stride=BITS), :] = (packed >> (16 + b)) & 1
            mask[tile, k, :, :LANES] = bits32[0, :CELLS].astype(F32).astype(BF16)
            mask[tile, k, :, LANES:] = bits32[1, :CELLS].astype(F32).astype(BF16)
        return carry

    lax.fori_loop(0, SLOTS, unpack, 0)

    nb_copy.wait_recv()

    def weight_wait(i, carry):
        chip = (f + i) % 16
        pltpu.make_async_copy(wall.at[chip], wall.at[chip], weight_sem.at[chip]).wait()
        return carry

    lax.fori_loop(1, 16, weight_wait, 0)
    kept = pl.ds(2 * core, 2)

    def forward_copy(w):
        return pltpu.make_async_remote_copy(
            win.at[w, :, kept], win.at[w, :, kept], fwd_send.at[w], fwd_sem.at[w],
            device_id=device(partner, f), device_id_type=MESH,
        )

    def forward(w, carry):
        from_here = (dest_row + w - 2) // 4 == t
        from_chip = (dest_row + w - 2) // 4 % 2 == core
        even = (dest_row + w) % 2 == 0

        @pl.when(jnp.logical_and(row_exists(w), even))
        def _():
            for source_x in range(4):

                @pl.when(jnp.logical_not(jnp.logical_and(from_chip, x == source_x)))
                def _():
                    piece = win.at[w, :, kept, source_x]
                    pltpu.make_async_copy(piece, piece, win_y_sem.at[w, source_x]).wait()

        @pl.when(jnp.logical_and(row_exists(w), jnp.logical_not(even)))
        def _():
            for side in range(2):

                @pl.when(jnp.logical_not(jnp.logical_and(from_here, y == 2 * core + side)))
                def _():
                    piece = win.at[w, :, 2 * core + side]
                    pltpu.make_async_copy(piece, piece, win_x_sem.at[w, side]).wait()

        @pl.when(row_exists(w))
        def _():
            forward_copy(w).start()

        return carry

    lax.fori_loop(0, WIN_ROWS, forward, 0)

    given = pl.ds(2 - 2 * core, 2)

    def turn_kept(w, carry):
        for c in range(WIN_COLS):
            feats_t[core, w * WIN_COLS + c, pl.ds(0, LANES)] = win[w, c, kept].reshape(LANES, LANES).T
        return carry

    lax.fori_loop(0, WIN_ROWS, turn_kept, 0)

    def turn_given(w, carry):
        @pl.when(row_exists(w))
        def _():
            forward_copy(w).wait_recv()

        for c in range(WIN_COLS):
            feats_t[1 - core, w * WIN_COLS + c, pl.ds(0, LANES)] = win[w, c, given].reshape(LANES, LANES).T
        return carry

    lax.fori_loop(0, WIN_ROWS, turn_given, 0)

    weight = wall[...].astype(F32).reshape(LANES, LANES).astype(BF16)
    bias = bias_ref[...]
    band = 2 * z + home

    firsts = 4 * (f % 8) + 2 * core
    rows = [
        jnp.clip(rows_ref[band * TILES + firsts + tile] - band * TILES, 0, TILES - 1) for tile in range(2)
    ]

    def add(k, totals):
        done = []
        for tile in range(2):
            near = jnp.where(home == core, nb_own[k, rows[tile]], nb_other[k, rows[tile]])
            place = (near // 8 - (dest_row - 2)) * WIN_COLS + near % 8 - 2 * half
            place = jnp.clip(place, 0, WIN_ROWS * WIN_COLS - 1)
            done.append(totals[tile] + jnp.dot(
                jnp.concatenate([feats_t[0, place], feats_t[1, place]], axis=1), mask[tile, k],
                preferred_element_type=F32,
            ))
        return tuple(done)

    zero = jnp.zeros((LANES + 16, CELLS), F32)
    totals = lax.fori_loop(0, SLOTS, add, (zero, zero), unroll=True)
    for tile in range(2):
        total = totals[tile].T
        base = win[2, 4 * half + 2 * core + tile - 2 * half].reshape(CELLS, LANES).astype(F32)
        degree = total[:, LANES : LANES + 1]
        normed = ((total[:, :LANES] + base) / jnp.sqrt(degree + 1.0)).astype(BF16)
        linear = jnp.dot(normed, weight, preferred_element_type=F32) + bias
        stage_o[tile] = (base + jnp.maximum(linear, 0.0)).astype(BF16)

    first_out = 4 * (f % 8) + 2 * core

    out_sends = []
    for i, chip in enumerate(chips):
        cells = pl.ds(pl.multiple_of(chip * CHUNK, CHUNK), CHUNK)
        copy = pltpu.make_async_remote_copy(
            stage_o.at[:, cells], obuf.at[pl.ds(first_out, 2)],
            out_send.at[i], out_sem.at[first_out // 2],
            device_id=device(2 * z + home, chip), device_id_type=MESH,
        )
        sent = home != core if STEPS[i] == (0, 0) else True
        out_sends.append((copy, sent))
        if sent is True:
            copy.start()
        else:
            pl.when(sent)(copy.start)

    @pl.when(home == core)
    def _():
        obuf[pl.ds(first_out, 2)] = stage_o[:, my_cells]

    nb_copy.wait_send()

    for copy, sent in word_sends:
        pl.when(sent)(copy.wait_send)

    def end_weight(i, carry):
        weight_copy(i).wait_send()
        return carry

    lax.fori_loop(1, 16, end_weight, 0)

    for copy, sent in first_sends + second_sends:
        if sent is True:
            copy.wait_send()
        else:
            pl.when(sent)(copy.wait_send)

    def end_forward(w, carry):
        @pl.when(row_exists(w))
        def _():
            forward_copy(w).wait_send()

        return carry

    lax.fori_loop(0, WIN_ROWS, end_forward, 0)

    for copy, sent in out_sends:
        if sent is True:
            copy.wait_send()
        else:
            pl.when(sent)(copy.wait_send)

    def arrive_out(i, carry):
        @pl.when(jnp.logical_not(jnp.logical_and(home == core, i == first_out // 2)))
        def _():
            pair = pl.ds(2 * i, 2)
            pltpu.make_async_copy(obuf.at[pair], obuf.at[pair], out_sem.at[i]).wait()

        return carry

    lax.fori_loop(0, 16, arrive_out, 0)

    def put(r, carry):
        out_ref[r] = obuf[inverse[r]]
        return carry

    lax.fori_loop(0, TILES, put, 0)


def solution(mesh):
    n_tiles = mesh.shape["tiles"]

    def per_device(feats, weight, bias, neighbours, counts, adj_words, tile_row):
        vmem = pl.BlockSpec(memory_space=pltpu.VMEM)
        hbm = pl.BlockSpec(memory_space=pl.ANY)
        words = adj_words.reshape(TILES, WORDS, CELLS)
        return pl.pallas_call(
            functools.partial(kernel, n_tiles),
            out_shape=pltpu.VMEM(feats.shape, BF16),
            in_specs=[hbm] * 7,
            out_specs=vmem,
            scratch_shapes=[
                pltpu.VMEM((TILES, CHUNK, LANES), BF16),
                pltpu.VMEM((TILES, WORDS, CELLS), I32),
                pltpu.VMEM((8, LANES), BF16),
                pltpu.VMEM((1, LANES), F32),
                pltpu.SMEM((TILES,), I32),
                pltpu.SMEM((n_tiles * TILES,), I32),
                pltpu.SMEM((SLOTS, TILES), I32),
                pltpu.SMEM((SLOTS, TILES), I32),
                pltpu.VMEM((4, 8, CHUNK, LANES), BF16),
                pltpu.VMEM((TILES, WORDS, LANES), I32),
                pltpu.VMEM((2, 8, 4, CHUNK, LANES), BF16),
                pltpu.VMEM((2, WIN_COLS, 4, CHUNK, LANES), BF16),
                pltpu.VMEM((WIN_ROWS, WIN_COLS, 4, 4, CHUNK, LANES), BF16),
                pltpu.VMEM((SLOTS, 2, WORDS, LANES), I32),
                pltpu.VMEM((16, 8, LANES), BF16),
                pltpu.VMEM((2, WORDS * BITS, LANES), I32),
                pltpu.VMEM((2, SLOTS, CELLS, CELLS), BF16),
                pltpu.VMEM((2, WIN_ROWS * WIN_COLS, LANES + 16, LANES), BF16),
                pltpu.VMEM((2, CELLS, LANES), BF16),
                pltpu.VMEM((TILES, CHUNK, LANES), BF16),
                pltpu.SMEM((TILES,), I32),
                pltpu.SemaphoreType.DMA((7,)),
                pltpu.SemaphoreType.DMA,
                pltpu.SemaphoreType.DMA,
                pltpu.SemaphoreType.DMA((32,)),
                pltpu.SemaphoreType.DMA((SLOTS,)),
                pltpu.SemaphoreType.DMA((16,)),
                pltpu.SemaphoreType.DMA((16,)),
                pltpu.SemaphoreType.DMA((2, 4)),
                pltpu.SemaphoreType.DMA((2, 4)),
                pltpu.SemaphoreType.DMA((2, 4)),
                pltpu.SemaphoreType.DMA((2, 4)),
                pltpu.SemaphoreType.DMA((2, 4, 2)),
                pltpu.SemaphoreType.DMA((WIN_ROWS, 4)),
                pltpu.SemaphoreType.DMA((2, 4)),
                pltpu.SemaphoreType.DMA((WIN_ROWS, 2)),
                pltpu.SemaphoreType.DMA((WIN_ROWS,)),
                pltpu.SemaphoreType.DMA((WIN_ROWS,)),
                pltpu.SemaphoreType.DMA((16,)),
                pltpu.SemaphoreType.DMA((16,)),
            ],
            compiler_params=pltpu.CompilerParams(collective_id=0, has_side_effects=True),
        )(feats, weight, bias.reshape(1, LANES), neighbours.T, words, counts, tile_row)

    return jax.shard_map(
        per_device,
        mesh=mesh,
        in_specs=(
            P("tiles", "feat", None),
            P("feat", None),
            P(),
            P("tiles", None),
            P("tiles"),
            P("tiles", "feat", None, None),
            P(),
        ),
        out_specs=P("tiles", "feat", None),
        check_vma=False,
    )
```

```python
import functools

import jax
import jax.numpy as jnp
from jax import lax
from jax.experimental import pallas as pl
from jax.experimental.pallas import tpu as pltpu
from jax.sharding import PartitionSpec as P

MESH = pl.DeviceIdType.MESH
STEPS = (
    (2, 2), (1, 2), (3, 2), (2, 1), (2, 3), (0, 2), (2, 0), (1, 1),
    (3, 3), (1, 3), (3, 1), (0, 1), (0, 3), (1, 0), (3, 0), (0, 0),
)
BF16 = jnp.bfloat16
F32 = jnp.float32
I32 = jnp.int32

SLOTS = 16
CELLS = 256
CHUNK = 16
WORDS = 24
BITS = 11
LANES = 128
TILES = 32
WIN_ROWS = 5
WIN_COLS = 6


def kernel(
    n_tiles,
    feats_hbm, weight_hbm, bias_hbm, nb_hbm, words_hbm, counts_hbm, rows_hbm,
    out_ref,
    feats_v, words_v, weight_v, bias_ref, counts_ref, rows_ref, nb_own, nb_other, stage_f, stage_w, relay_y, relay_x, win, wbuf, wall, bits32, mask, feats_t, stage_o, obuf, inverse,
    local_sem, nb_send, nb_sem, word_send, word_sem, weight_send, weight_sem, to_y_send, to_y_sem, to_x_send, to_x_sem, win_y_send, win_x_send, win_sem, fwd_send, fwd_sem, out_send, out_sem,
):
    t = lax.axis_index("tiles")
    f = lax.axis_index("feat")
    z = t // 2
    core = t % 2
    partner = 2 * z + 1 - core
    row_in_plane = f // 2
    y, x = f // 4, f % 4
    half = f % 2
    home = f // 8
    dest_row = 8 * z + row_in_plane
    n_planes = n_tiles // 2

    def device(tiles, feat):
        return {"tiles": tiles, "feat": feat}

    def settle(sem, piece):
        pltpu.make_async_copy(piece, piece, sem).wait()

    def settle_count(sem, sent, most, pieces):
        count = sum(jnp.asarray(one).astype(I32) for one in sent)
        for n in range(1, most + 1):

            @pl.when(count == n)
            def _():
                settle(sem, pieces(n))

    loads = [
        pltpu.make_async_copy(words_hbm, words_v, local_sem.at[0]),
        pltpu.make_async_copy(feats_hbm, feats_v, local_sem.at[1]),
        pltpu.make_async_copy(weight_hbm, weight_v, local_sem.at[2]),
        pltpu.make_async_copy(nb_hbm, nb_own, local_sem.at[3]),
        pltpu.make_async_copy(bias_hbm, bias_ref, local_sem.at[4]),
        pltpu.make_async_copy(counts_hbm, counts_ref, local_sem.at[5]),
        pltpu.make_async_copy(rows_hbm, rows_ref, local_sem.at[6]),
    ]
    for load in loads:
        load.start()

    barrier = pltpu.get_barrier_semaphore()

    chips = [(f // 4 + dy) % 4 * 4 + (f % 4 + dx) % 4 for dy, dx in STEPS]

    for i, chip in enumerate(chips):
        for tiles in (partner,) if STEPS[i] == (0, 0) else (t, partner):
            pl.semaphore_signal(barrier, inc=1, device_id=device(tiles, chip), device_id_type=MESH)

    def plane_for(chip_y):
        below = jnp.logical_and(core == 0, chip_y == 3).astype(I32)
        above = jnp.logical_and(core == 1, chip_y == 0).astype(I32)
        return z - below + above

    def ahead_of(chip_y):
        return (2 * chip_y + jnp.where(core == 0, 2, 6)) % 8 - 2

    def in_slide(plane):
        return jnp.logical_and(plane >= 0, plane < n_planes)

    for source_y in range(4):
        above = jnp.logical_and(y == 3, z < n_planes - 1)
        below = jnp.logical_and(y == 0, z > 0)
        if source_y < 2:
            above = jnp.logical_and(above, core == 0)
        else:
            below = jnp.logical_and(below, core == 1)

        @pl.when(above)
        def _():
            pl.semaphore_signal(
                barrier, inc=1, device_id=device(2 * z + 2, 4 * source_y + x), device_id_type=MESH
            )

        @pl.when(below)
        def _():
            pl.semaphore_signal(
                barrier, inc=1, device_id=device(2 * z - 1, 4 * source_y + x), device_id_type=MESH
            )

    for load in loads:
        load.wait()

    def order(s, carry):
        row = jnp.clip(rows_ref[t * TILES + s] - t * TILES, 0, TILES - 1)
        live = f < counts_ref[row]
        w = words_v[row]
        packed = w[:, :LANES] | (w[:, LANES:] << 16)
        stage_w[s] = jnp.where(live, packed, jnp.zeros_like(packed))
        stage_f[s // 8, s % 8] = feats_v[row]
        return carry

    lax.fori_loop(0, TILES, order, 0)

    beyond = jnp.where(
        core == 0, jnp.where(z > 0, 1 + y // 2, 0), jnp.where(z < n_planes - 1, 2 - y // 2, 0)
    )
    for peers in range(3):

        @pl.when(beyond == peers)
        def _():
            pl.semaphore_wait(barrier, 31 + peers)

    first_y, first_x, second_y, second_x = ([], []), [], [], []

    def reaches(r, ahead):
        return jnp.logical_and(ahead >= r - 3, ahead <= r + 2)

    def send(copy, sent, sends):
        sends.append(sent)
        if sent is True:
            copy.start()
        else:
            pl.when(sent)(copy.start)

    for step in (2, 1, 3, 0):
        to_y = (y + step) % 4
        plane = plane_for(to_y)
        for i in range(2):
            sent = jnp.logical_and(in_slide(plane), reaches(2 * i, ahead_of(to_y)))
            if step == 0:
                mine = jnp.logical_and(sent, plane == z)
                sent = jnp.logical_and(sent, plane != z)

                @pl.when(mine)
                def _():
                    relay_y[i, :, y] = stage_f[2 * i]

            copy = pltpu.make_async_remote_copy(
                stage_f.at[2 * i], relay_y.at[i, :, y], to_y_send.at[i], to_y_sem.at[i],
                device_id=device(2 * plane + core, 4 * to_y + x), device_id_type=MESH,
            )
            send(copy, sent, first_y[i])
        to_x = (x + step) % 4
        for i in range(2):
            columns = pl.ds(2 * (to_x % 2), WIN_COLS)
            if step == 0:
                relay_x[i, :, x] = stage_f[2 * i + 1, columns]
            else:
                copy = pltpu.make_async_remote_copy(
                    stage_f.at[2 * i + 1, columns], relay_x.at[i, :, x],
                    to_x_send, to_x_sem.at[i],
                    device_id=device(t, 4 * y + to_x), device_id_type=MESH,
                )
                send(copy, True, first_x)

    nb_copy = pltpu.make_async_remote_copy(
        nb_own, nb_other, nb_send, nb_sem, device_id=device(partner, f), device_id_type=MESH
    )
    nb_copy.start()

    word_sends = []
    for i, chip in enumerate(chips):
        for side in range(2):
            sent = chip // 8 == core
            if STEPS[i] == (0, 0):
                sent = jnp.logical_and(sent, side != core)
            copy = pltpu.make_async_remote_copy(
                stage_w.at[pl.ds(4 * (chip % 8) + 2 * side, 2)], wbuf.at[f],
                word_send, word_sem.at[f // 4],
                device_id=device(2 * z + side, chip), device_id_type=MESH,
            )
            word_sends.append(sent)
            pl.when(sent)(copy.start)

    @pl.when(home == core)
    def _():
        wbuf[f] = stage_w[pl.ds(4 * (f % 8) + 2 * core, 2)]

    weight_mine = weight_v[...]
    wall[f] = weight_mine

    def weight_copy(i):
        chip = (f + i) % 16
        return pltpu.make_async_remote_copy(
            weight_v, wall.at[f], weight_send, weight_sem,
            device_id=device(t, chip), device_id_type=MESH,
        )

    def start_weight(i, carry):
        weight_copy(i).start()
        return carry

    lax.fori_loop(1, 16, start_weight, 0)

    def row_exists(w):
        row = dest_row + w - 2
        return jnp.logical_and(row >= 0, row < 4 * n_tiles)

    def clear(w, carry):
        @pl.when(jnp.logical_not(row_exists(w)))
        def _():
            win[w] = jnp.zeros((WIN_COLS, 4, 4, CHUNK, LANES), BF16)

        return carry

    lax.fori_loop(0, WIN_ROWS, clear, 0)

    ones_rows = jnp.ones((16, LANES), BF16)

    def fill_ones(i, carry):
        feats_t[0, i, pl.ds(LANES, 16)] = ones_rows
        feats_t[1, i, pl.ds(LANES, 16)] = ones_rows
        return carry

    lax.fori_loop(0, WIN_ROWS * WIN_COLS, fill_ones, 0)

    my_cells = pl.ds(pl.multiple_of(f * CHUNK, CHUNK), CHUNK)
    ahead = ahead_of(y)
    band_plane = z + jnp.logical_and(core == 0, y == 3).astype(I32) - jnp.logical_and(
        core == 1, y == 0).astype(I32)

    for i in range(2):
        r = 2 * i
        here = jnp.logical_and(in_slide(band_plane), reaches(r, ahead))

        @pl.when(jnp.logical_and(here, band_plane != z))
        def _():
            settle(to_y_sem.at[i], relay_y.at[i])

        @pl.when(jnp.logical_and(here, band_plane == z))
        def _():
            settle(to_y_sem.at[i], relay_y.at[i, :, pl.ds(0, 3)])

        for step in (2, 1, 3, 0):
            to_x = (x + step) % 4
            gap = ahead + to_x // 2 - r
            w = jnp.clip(2 - gap, 0, WIN_ROWS - 1)
            columns = pl.ds(2 * (to_x % 2), WIN_COLS)
            needed = jnp.logical_and(here, jnp.logical_and(gap >= -2, gap <= 2))
            for q in range(2):
                sent = needed
                if step == 0:
                    sent = jnp.logical_and(needed, core != q)

                    @pl.when(jnp.logical_and(needed, core == q))
                    def _():
                        win[w, :, 2 * q : 2 * q + 2, x] = relay_y[i, columns, 2 * q : 2 * q + 2]

                copy = pltpu.make_async_remote_copy(
                    relay_y.at[i, columns, pl.ds(2 * q, 2)], win.at[w, :, pl.ds(2 * q, 2), x],
                    win_y_send, win_sem.at[w],
                    device_id=device(2 * z + q, 4 * y + to_x), device_id_type=MESH,
                )
                send(copy, sent, second_y)

        r = 2 * i + 1
        settle(to_x_sem.at[i], relay_x.at[i, :, pl.ds(0, 3)])

        for step in (2, 1, 3, 0):
            to_y = (y + step) % 4
            plane = plane_for(to_y)
            gap = ahead_of(to_y) + x // 2 - r
            w = jnp.clip(2 - gap, 0, WIN_ROWS - 1)
            sent = jnp.logical_and(in_slide(plane), jnp.logical_and(gap >= -2, gap <= 2))
            if step == 0:
                at_home = jnp.logical_and(plane == z, home == core)
                mine = jnp.logical_and(sent, at_home)
                sent = jnp.logical_and(sent, jnp.logical_not(at_home))

                @pl.when(mine)
                def _():
                    win[w, :, y] = relay_x[i]

            copy = pltpu.make_async_remote_copy(
                relay_x.at[i], win.at[w, :, y], win_x_send, win_sem.at[w],
                device_id=device(2 * plane + home, 4 * to_y + x), device_id_type=MESH,
            )
            send(copy, sent, second_x)

    def invert(r, carry):
        found = 0
        for s in range(1, TILES):
            found = found + jnp.where(rows_ref[t * TILES + s] == t * TILES + r, s, 0)
        inverse[r] = jnp.clip(found, 0, TILES - 1)
        return carry

    lax.fori_loop(0, TILES, invert, 0)

    def unpack(k, carry):
        with_mine = jnp.logical_and(k == f // 4 * 4, core == home)

        @pl.when(with_mine)
        def _():
            settle(word_sem.at[k // 4], wbuf.at[pl.ds(k, 3)])

        @pl.when(jnp.logical_and(k % 4 == 0, jnp.logical_not(with_mine)))
        def _():
            settle(word_sem.at[k // 4], wbuf.at[pl.ds(k, 4)])

        for tile in range(2):
            packed = wbuf[k, tile]
            for b in range(BITS):
                bits32[0, pl.ds(b, WORDS, stride=BITS), :] = (packed >> b) & 1
                bits32[1, pl.ds(b, WORDS, stride=BITS), :] = (packed >> (16 + b)) & 1
            mask[tile, k, :, :LANES] = bits32[0, :CELLS].astype(F32).astype(BF16)
            mask[tile, k, :, LANES:] = bits32[1, :CELLS].astype(F32).astype(BF16)
        return carry

    lax.fori_loop(0, SLOTS, unpack, 0)

    nb_copy.wait_recv()

    settle(weight_sem, wall.at[pl.ds(0, 15)])
    kept = pl.ds(2 * core, 2)

    def forward_copy(w):
        return pltpu.make_async_remote_copy(
            win.at[w, :, kept], win.at[w, :, kept], fwd_send, fwd_sem.at[w],
            device_id=device(partner, f), device_id_type=MESH,
        )

    def forward(w, carry):
        from_here = (dest_row + w - 2) // 4 == t
        from_chip = (dest_row + w - 2) // 4 % 2 == core
        even = (dest_row + w) % 2 == 0

        part_here = jnp.where(even, from_chip, jnp.logical_and(from_here, home == core))

        @pl.when(jnp.logical_and(row_exists(w), jnp.logical_not(part_here)))
        def _():
            settle(win_sem.at[w], win.at[w, :, kept])

        @pl.when(jnp.logical_and(row_exists(w), jnp.logical_and(part_here, even)))
        def _():
            settle(win_sem.at[w], win.at[w, :, kept, pl.ds(0, 3)])

        @pl.when(jnp.logical_and(row_exists(w), jnp.logical_and(part_here, jnp.logical_not(even))))
        def _():
            settle(win_sem.at[w], win.at[w, :, 2 * core])

        @pl.when(row_exists(w))
        def _():
            forward_copy(w).start()

        return carry

    lax.fori_loop(0, WIN_ROWS, forward, 0)

    given = pl.ds(2 - 2 * core, 2)

    def turn_kept(w, carry):
        for c in range(WIN_COLS):
            feats_t[core, w * WIN_COLS + c, pl.ds(0, LANES)] = win[w, c, kept].reshape(LANES, LANES).T
        return carry

    lax.fori_loop(0, WIN_ROWS, turn_kept, 0)

    def turn_given(w, carry):
        @pl.when(row_exists(w))
        def _():
            forward_copy(w).wait_recv()

        for c in range(WIN_COLS):
            feats_t[1 - core, w * WIN_COLS + c, pl.ds(0, LANES)] = win[w, c, given].reshape(LANES, LANES).T
        return carry

    lax.fori_loop(0, WIN_ROWS, turn_given, 0)

    weight = wall[...].astype(F32).reshape(LANES, LANES).astype(BF16)
    bias = bias_ref[...]
    band = 2 * z + home

    firsts = 4 * (f % 8) + 2 * core
    rows = [
        jnp.clip(rows_ref[band * TILES + firsts + tile] - band * TILES, 0, TILES - 1) for tile in range(2)
    ]

    def add(k, totals):
        done = []
        for tile in range(2):
            near = jnp.where(home == core, nb_own[k, rows[tile]], nb_other[k, rows[tile]])
            place = (near // 8 - (dest_row - 2)) * WIN_COLS + near % 8 - 2 * half
            place = jnp.clip(place, 0, WIN_ROWS * WIN_COLS - 1)
            done.append(totals[tile] + jnp.dot(
                jnp.concatenate([feats_t[0, place], feats_t[1, place]], axis=1), mask[tile, k],
                preferred_element_type=F32,
            ))
        return tuple(done)

    zero = jnp.zeros((LANES + 16, CELLS), F32)
    totals = lax.fori_loop(0, SLOTS, add, (zero, zero), unroll=True)
    for tile in range(2):
        total = totals[tile].T
        base = win[2, 4 * half + 2 * core + tile - 2 * half].reshape(CELLS, LANES).astype(F32)
        degree = total[:, LANES : LANES + 1]
        normed = ((total[:, :LANES] + base) / jnp.sqrt(degree + 1.0)).astype(BF16)
        linear = jnp.dot(normed, weight, preferred_element_type=F32) + bias
        stage_o[tile] = (base + jnp.maximum(linear, 0.0)).astype(BF16)

    first_out = 4 * (f % 8) + 2 * core

    for i, chip in enumerate(chips):
        cells = pl.ds(pl.multiple_of(chip * CHUNK, CHUNK), CHUNK)
        copy = pltpu.make_async_remote_copy(
            stage_o.at[:, cells], obuf.at[pl.ds(first_out, 2)],
            out_send, out_sem,
            device_id=device(2 * z + home, chip), device_id_type=MESH,
        )
        sent = home != core if STEPS[i] == (0, 0) else True
        if sent is True:
            copy.start()
        else:
            pl.when(sent)(copy.start)

    @pl.when(home == core)
    def _():
        obuf[pl.ds(first_out, 2)] = stage_o[:, my_cells]

    nb_copy.wait_send()
    settle(weight_send, wall.at[pl.ds(0, 15)])
    for i in range(2):
        settle_count(to_y_send.at[i], first_y[i], 3, lambda n: relay_y.at[0, :, pl.ds(0, n)])
    settle(to_x_send, relay_x.at[:, :, pl.ds(0, 3)])
    settle_count(win_y_send, second_y, 16, lambda n: words_v.at[pl.ds(0, 2 * n)])
    settle_count(win_x_send, second_x, 8, lambda n: words_v.at[pl.ds(0, 4 * n)])
    settle_count(
        fwd_send, [row_exists(w) for w in range(WIN_ROWS)], WIN_ROWS, lambda n: win.at[pl.ds(0, n), :, kept]
    )

    @pl.when(home == core)
    def _():
        settle(word_send, stage_w.at[pl.ds(0, 30)])
        settle(out_send, obuf.at[pl.ds(0, 30)])

    @pl.when(home != core)
    def _():
        settle(word_send, stage_w)
        settle(out_send, obuf)

    @pl.when(home == core)
    def _():
        settle(out_sem, obuf.at[pl.ds(0, 30)])

    @pl.when(home != core)
    def _():
        settle(out_sem, obuf)

    def put(r, carry):
        out_ref[r] = obuf[inverse[r]]
        return carry

    lax.fori_loop(0, TILES, put, 0)


def solution(mesh):
    n_tiles = mesh.shape["tiles"]

    def per_device(feats, weight, bias, neighbours, counts, adj_words, tile_row):
        vmem = pl.BlockSpec(memory_space=pltpu.VMEM)
        hbm = pl.BlockSpec(memory_space=pl.ANY)
        words = adj_words.reshape(TILES, WORDS, CELLS)
        return pl.pallas_call(
            functools.partial(kernel, n_tiles),
            out_shape=pltpu.VMEM(feats.shape, BF16),
            in_specs=[hbm] * 7,
            out_specs=vmem,
            scratch_shapes=[
                pltpu.VMEM((TILES, CHUNK, LANES), BF16),
                pltpu.VMEM((TILES, WORDS, CELLS), I32),
                pltpu.VMEM((8, LANES), BF16),
                pltpu.VMEM((1, LANES), F32),
                pltpu.SMEM((TILES,), I32),
                pltpu.SMEM((n_tiles * TILES,), I32),
                pltpu.SMEM((SLOTS, TILES), I32),
                pltpu.SMEM((SLOTS, TILES), I32),
                pltpu.VMEM((4, 8, CHUNK, LANES), BF16),
                pltpu.VMEM((TILES, WORDS, LANES), I32),
                pltpu.VMEM((2, 8, 4, CHUNK, LANES), BF16),
                pltpu.VMEM((2, WIN_COLS, 4, CHUNK, LANES), BF16),
                pltpu.VMEM((WIN_ROWS, WIN_COLS, 4, 4, CHUNK, LANES), BF16),
                pltpu.VMEM((SLOTS, 2, WORDS, LANES), I32),
                pltpu.VMEM((16, 8, LANES), BF16),
                pltpu.VMEM((2, WORDS * BITS, LANES), I32),
                pltpu.VMEM((2, SLOTS, CELLS, CELLS), BF16),
                pltpu.VMEM((2, WIN_ROWS * WIN_COLS, LANES + 16, LANES), BF16),
                pltpu.VMEM((2, CELLS, LANES), BF16),
                pltpu.VMEM((TILES, CHUNK, LANES), BF16),
                pltpu.SMEM((TILES,), I32),
                pltpu.SemaphoreType.DMA((7,)),
                pltpu.SemaphoreType.DMA,
                pltpu.SemaphoreType.DMA,
                pltpu.SemaphoreType.DMA,
                pltpu.SemaphoreType.DMA((4,)),
                pltpu.SemaphoreType.DMA,
                pltpu.SemaphoreType.DMA,
                pltpu.SemaphoreType.DMA((2,)),
                pltpu.SemaphoreType.DMA((2,)),
                pltpu.SemaphoreType.DMA,
                pltpu.SemaphoreType.DMA((2,)),
                pltpu.SemaphoreType.DMA,
                pltpu.SemaphoreType.DMA,
                pltpu.SemaphoreType.DMA((WIN_ROWS,)),
                pltpu.SemaphoreType.DMA,
                pltpu.SemaphoreType.DMA((WIN_ROWS,)),
                pltpu.SemaphoreType.DMA,
                pltpu.SemaphoreType.DMA,
            ],
            compiler_params=pltpu.CompilerParams(collective_id=0, has_side_effects=True),
        )(feats, weight, bias.reshape(1, LANES), neighbours.T, words, counts, tile_row)

    return jax.shard_map(
        per_device,
        mesh=mesh,
        in_specs=(
            P("tiles", "feat", None),
            P("feat", None),
            P(),
            P("tiles", None),
            P("tiles"),
            P("tiles", "feat", None, None),
            P(),
        ),
        out_specs=P("tiles", "feat", None),
        check_vma=False,
    )
```

```python
import functools

import jax
import jax.numpy as jnp
from jax import lax
from jax.experimental import pallas as pl
from jax.experimental.pallas import tpu as pltpu
from jax.sharding import PartitionSpec as P

MESH = pl.DeviceIdType.MESH
STEPS = (
    (2, 2), (1, 2), (3, 2), (2, 1), (2, 3), (0, 2), (2, 0), (1, 1),
    (3, 3), (1, 3), (3, 1), (0, 1), (0, 3), (1, 0), (3, 0), (0, 0),
)
BF16 = jnp.bfloat16
F32 = jnp.float32
I32 = jnp.int32

SLOTS = 16
CELLS = 256
CHUNK = 16
WORDS = 24
BITS = 11
LANES = 128
TILES = 32
WIN_ROWS = 5
WIN_COLS = 6


def kernel(
    n_tiles,
    feats_hbm, weight_hbm, bias_hbm, nb_hbm, words_hbm, counts_hbm, rows_hbm,
    out_ref,
    feats_v, words_v, weight_v, bias_ref, counts_ref, rows_ref, nb_own, nb_other, stage_f, stage_w, relay_y, relay_x, win, wbuf, wall, bits32, mask, feats_t, stage_o, obuf, inverse,
    local_sem, met_sem, nb_send, nb_sem, word_send, word_sem, weight_send, weight_sem, to_y_send, to_y_sem, to_x_send, to_x_sem, win_y_send, win_x_send, win_sem, fwd_send, fwd_sem, out_send, out_sem,
):
    t = lax.axis_index("tiles")
    f = lax.axis_index("feat")
    z = t // 2
    core = t % 2
    partner = 2 * z + 1 - core
    row_in_plane = f // 2
    y, x = f // 4, f % 4
    half = f % 2
    home = f // 8
    dest_row = 8 * z + row_in_plane
    n_planes = n_tiles // 2

    def device(tiles, feat):
        return {"tiles": tiles, "feat": feat}

    def settle(sem, piece):
        pltpu.make_async_copy(piece, piece, sem).wait()

    def settle_count(sem, sent, most, pieces):
        count = sum(jnp.asarray(one).astype(I32) for one in sent)
        for n in range(1, most + 1):

            @pl.when(count == n)
            def _():
                settle(sem, pieces(n))

    early = [
        pltpu.make_async_copy(rows_hbm, rows_ref, local_sem.at[0]),
        pltpu.make_async_copy(feats_hbm, feats_v, local_sem.at[1]),
    ]
    late = [
        pltpu.make_async_copy(words_hbm, words_v, local_sem.at[2]),
        pltpu.make_async_copy(counts_hbm, counts_ref, local_sem.at[3]),
        pltpu.make_async_copy(nb_hbm, nb_own, local_sem.at[4]),
        pltpu.make_async_copy(weight_hbm, weight_v, local_sem.at[5]),
        pltpu.make_async_copy(bias_hbm, bias_ref, local_sem.at[6]),
    ]
    for load in early:
        load.start()

    barrier = pltpu.get_barrier_semaphore()

    chips = [(f // 4 + dy) % 4 * 4 + (f % 4 + dx) % 4 for dy, dx in STEPS]

    for (dy, dx), chip in zip(STEPS, chips):
        if dy * dx == 0:
            for tiles in (partner,) if (dy, dx) == (0, 0) else (t, partner):
                pl.semaphore_signal(barrier, inc=1, device_id=device(tiles, chip), device_id_type=MESH)

    @pl.when(z > 0)
    def _():
        pl.semaphore_signal(barrier, inc=1, device_id=device(t - 2, f), device_id_type=MESH)

    @pl.when(z < n_planes - 1)
    def _():
        pl.semaphore_signal(barrier, inc=1, device_id=device(t + 2, f), device_id_type=MESH)

    for load in late:
        load.start()

    def plane_for(chip_y):
        below = jnp.logical_and(core == 0, chip_y == 3).astype(I32)
        above = jnp.logical_and(core == 1, chip_y == 0).astype(I32)
        return z - below + above

    def ahead_of(chip_y):
        return (2 * chip_y + jnp.where(core == 0, 2, 6)) % 8 - 2

    def in_slide(plane):
        return jnp.logical_and(plane >= 0, plane < n_planes)

    for load in early:
        load.wait()

    def own_row(s):
        return jnp.clip(rows_ref[t * TILES + s] - t * TILES, 0, TILES - 1)

    for s in range(TILES):
        stage_f[s // 8, s % 8] = feats_v[own_row(s)]

    at_end = jnp.logical_or(z == 0, z == n_planes - 1)

    @pl.when(at_end)
    def _():
        pl.semaphore_wait(barrier, 14)

    @pl.when(jnp.logical_not(at_end))
    def _():
        pl.semaphore_wait(barrier, 15)

    for step in (2, 1, 3):
        pl.semaphore_signal(
            met_sem, inc=1, device_id=device(t, (y + step) % 4 * 4 + x), device_id_type=MESH
        )

    @pl.when(jnp.logical_and(core == 0, z < n_planes - 1))
    def _():
        pl.semaphore_signal(met_sem, inc=1, device_id=device(t + 2, f), device_id_type=MESH)

    @pl.when(jnp.logical_and(core == 1, z > 0))
    def _():
        pl.semaphore_signal(met_sem, inc=1, device_id=device(t - 2, f), device_id_type=MESH)

    first_y, first_x, second_y, second_x = ([], []), [], [], []

    def reaches(r, ahead):
        return jnp.logical_and(ahead >= r - 3, ahead <= r + 2)

    def send(copy, sent, sends):
        sends.append(sent)
        if sent is True:
            copy.start()
        else:
            pl.when(sent)(copy.start)

    def first_along_y(step, i, in_plane):
        to_y = (y + step) % 4
        plane = plane_for(to_y)
        sent = jnp.logical_and(in_slide(plane), reaches(2 * i, ahead_of(to_y)))
        sent = jnp.logical_and(sent, (plane == z) == in_plane)
        if in_plane and step == 0:

            @pl.when(sent)
            def _():
                relay_y[i, :, y] = stage_f[2 * i]

            return
        copy = pltpu.make_async_remote_copy(
            stage_f.at[2 * i], relay_y.at[i, :, y], to_y_send.at[i], to_y_sem.at[i],
            device_id=device(2 * plane + core, 4 * to_y + x), device_id_type=MESH,
        )
        send(copy, sent, first_y[i])

    for step in (2, 1, 3, 0):
        for i in range(2):
            first_along_y(step, i, True)
        to_x = (x + step) % 4
        for i in range(2):
            columns = pl.ds(2 * (to_x % 2), WIN_COLS)
            if step == 0:
                relay_x[i, :, x] = stage_f[2 * i + 1, columns]
            else:
                copy = pltpu.make_async_remote_copy(
                    stage_f.at[2 * i + 1, columns], relay_x.at[i, :, x],
                    to_x_send, to_x_sem.at[i],
                    device_id=device(t, 4 * y + to_x), device_id_type=MESH,
                )
                send(copy, True, first_x)

    for load in late:
        load.wait()

    def order_words(s, carry):
        row = own_row(s)
        live = f < counts_ref[row]
        w = words_v[row]
        packed = w[:, :LANES] | (w[:, LANES:] << 16)
        stage_w[s] = jnp.where(live, packed, jnp.zeros_like(packed))
        return carry

    lax.fori_loop(0, TILES, order_words, 0)

    meets_beyond = jnp.where(core == 0, z > 0, z < n_planes - 1)

    @pl.when(meets_beyond)
    def _():
        pl.semaphore_wait(met_sem, 4)

    @pl.when(jnp.logical_not(meets_beyond))
    def _():
        pl.semaphore_wait(met_sem, 3)

    for step in (2, 1, 3, 0):
        for i in range(2):
            first_along_y(step, i, False)

    nb_copy = pltpu.make_async_remote_copy(
        nb_own, nb_other, nb_send, nb_sem, device_id=device(partner, f), device_id_type=MESH
    )
    nb_copy.start()

    word_sends = []
    for i, chip in enumerate(chips):
        for side in range(2):
            sent = chip // 8 == core
            if STEPS[i] == (0, 0):
                sent = jnp.logical_and(sent, side != core)
            copy = pltpu.make_async_remote_copy(
                stage_w.at[pl.ds(4 * (chip % 8) + 2 * side, 2)], wbuf.at[f],
                word_send, word_sem.at[f // 4],
                device_id=device(2 * z + side, chip), device_id_type=MESH,
            )
            word_sends.append(sent)
            pl.when(sent)(copy.start)

    @pl.when(home == core)
    def _():
        wbuf[f] = stage_w[pl.ds(4 * (f % 8) + 2 * core, 2)]

    weight_mine = weight_v[...]
    wall[f] = weight_mine

    def weight_copy(i):
        chip = (f + i) % 16
        return pltpu.make_async_remote_copy(
            weight_v, wall.at[f], weight_send, weight_sem,
            device_id=device(t, chip), device_id_type=MESH,
        )

    def start_weight(i, carry):
        weight_copy(i).start()
        return carry

    lax.fori_loop(1, 16, start_weight, 0)

    def row_exists(w):
        row = dest_row + w - 2
        return jnp.logical_and(row >= 0, row < 4 * n_tiles)

    def clear(w, carry):
        @pl.when(jnp.logical_not(row_exists(w)))
        def _():
            win[w] = jnp.zeros((WIN_COLS, 4, 4, CHUNK, LANES), BF16)

        return carry

    lax.fori_loop(0, WIN_ROWS, clear, 0)

    ones_rows = jnp.ones((16, LANES), BF16)

    def fill_ones(i, carry):
        feats_t[0, i, pl.ds(LANES, 16)] = ones_rows
        feats_t[1, i, pl.ds(LANES, 16)] = ones_rows
        return carry

    lax.fori_loop(0, WIN_ROWS * WIN_COLS, fill_ones, 0)

    my_cells = pl.ds(pl.multiple_of(f * CHUNK, CHUNK), CHUNK)
    ahead = ahead_of(y)
    band_plane = z + jnp.logical_and(core == 0, y == 3).astype(I32) - jnp.logical_and(
        core == 1, y == 0).astype(I32)

    for i in range(2):
        r = 2 * i
        here = jnp.logical_and(in_slide(band_plane), reaches(r, ahead))

        @pl.when(jnp.logical_and(here, band_plane != z))
        def _():
            settle(to_y_sem.at[i], relay_y.at[i])

        @pl.when(jnp.logical_and(here, band_plane == z))
        def _():
            settle(to_y_sem.at[i], relay_y.at[i, :, pl.ds(0, 3)])

        for step in (2, 1, 3, 0):
            to_x = (x + step) % 4
            gap = ahead + to_x // 2 - r
            w = jnp.clip(2 - gap, 0, WIN_ROWS - 1)
            columns = pl.ds(2 * (to_x % 2), WIN_COLS)
            needed = jnp.logical_and(here, jnp.logical_and(gap >= -2, gap <= 2))
            for q in range(2):
                sent = needed
                if step == 0:
                    sent = jnp.logical_and(needed, core != q)

                    @pl.when(jnp.logical_and(needed, core == q))
                    def _():
                        win[w, :, 2 * q : 2 * q + 2, x] = relay_y[i, columns, 2 * q : 2 * q + 2]

                copy = pltpu.make_async_remote_copy(
                    relay_y.at[i, columns, pl.ds(2 * q, 2)], win.at[w, :, pl.ds(2 * q, 2), x],
                    win_y_send, win_sem.at[w],
                    device_id=device(2 * z + q, 4 * y + to_x), device_id_type=MESH,
                )
                send(copy, sent, second_y)

        r = 2 * i + 1
        settle(to_x_sem.at[i], relay_x.at[i, :, pl.ds(0, 3)])

        for step in (2, 1, 3, 0):
            to_y = (y + step) % 4
            plane = plane_for(to_y)
            gap = ahead_of(to_y) + x // 2 - r
            w = jnp.clip(2 - gap, 0, WIN_ROWS - 1)
            sent = jnp.logical_and(in_slide(plane), jnp.logical_and(gap >= -2, gap <= 2))
            if step == 0:
                at_home = jnp.logical_and(plane == z, home == core)
                mine = jnp.logical_and(sent, at_home)
                sent = jnp.logical_and(sent, jnp.logical_not(at_home))

                @pl.when(mine)
                def _():
                    win[w, :, y] = relay_x[i]

            copy = pltpu.make_async_remote_copy(
                relay_x.at[i], win.at[w, :, y], win_x_send, win_sem.at[w],
                device_id=device(2 * plane + home, 4 * to_y + x), device_id_type=MESH,
            )
            send(copy, sent, second_x)

    def invert(r, carry):
        found = 0
        for s in range(1, TILES):
            found = found + jnp.where(rows_ref[t * TILES + s] == t * TILES + r, s, 0)
        inverse[r] = jnp.clip(found, 0, TILES - 1)
        return carry

    lax.fori_loop(0, TILES, invert, 0)

    def unpack(k, carry):
        with_mine = jnp.logical_and(k == f // 4 * 4, core == home)

        @pl.when(with_mine)
        def _():
            settle(word_sem.at[k // 4], wbuf.at[pl.ds(k, 3)])

        @pl.when(jnp.logical_and(k % 4 == 0, jnp.logical_not(with_mine)))
        def _():
            settle(word_sem.at[k // 4], wbuf.at[pl.ds(k, 4)])

        for tile in range(2):
            packed = wbuf[k, tile]
            for b in range(BITS):
                bits32[0, pl.ds(b, WORDS, stride=BITS), :] = (packed >> b) & 1
                bits32[1, pl.ds(b, WORDS, stride=BITS), :] = (packed >> (16 + b)) & 1
            mask[tile, k, :, :LANES] = bits32[0, :CELLS].astype(F32).astype(BF16)
            mask[tile, k, :, LANES:] = bits32[1, :CELLS].astype(F32).astype(BF16)
        return carry

    lax.fori_loop(0, SLOTS, unpack, 0)

    nb_copy.wait_recv()

    settle(weight_sem, wall.at[pl.ds(0, 15)])
    kept = pl.ds(2 * core, 2)

    def forward_copy(w):
        return pltpu.make_async_remote_copy(
            win.at[w, :, kept], win.at[w, :, kept], fwd_send, fwd_sem.at[w],
            device_id=device(partner, f), device_id_type=MESH,
        )

    def forward(w, carry):
        from_here = (dest_row + w - 2) // 4 == t
        from_chip = (dest_row + w - 2) // 4 % 2 == core
        even = (dest_row + w) % 2 == 0

        part_here = jnp.where(even, from_chip, jnp.logical_and(from_here, home == core))

        @pl.when(jnp.logical_and(row_exists(w), jnp.logical_not(part_here)))
        def _():
            settle(win_sem.at[w], win.at[w, :, kept])

        @pl.when(jnp.logical_and(row_exists(w), jnp.logical_and(part_here, even)))
        def _():
            settle(win_sem.at[w], win.at[w, :, kept, pl.ds(0, 3)])

        @pl.when(jnp.logical_and(row_exists(w), jnp.logical_and(part_here, jnp.logical_not(even))))
        def _():
            settle(win_sem.at[w], win.at[w, :, 2 * core])

        @pl.when(row_exists(w))
        def _():
            forward_copy(w).start()

        return carry

    lax.fori_loop(0, WIN_ROWS, forward, 0)

    given = pl.ds(2 - 2 * core, 2)

    def turn_kept(w, carry):
        for c in range(WIN_COLS):
            feats_t[core, w * WIN_COLS + c, pl.ds(0, LANES)] = win[w, c, kept].reshape(LANES, LANES).T
        return carry

    lax.fori_loop(0, WIN_ROWS, turn_kept, 0)

    def turn_given(w, carry):
        @pl.when(row_exists(w))
        def _():
            forward_copy(w).wait_recv()

        for c in range(WIN_COLS):
            feats_t[1 - core, w * WIN_COLS + c, pl.ds(0, LANES)] = win[w, c, given].reshape(LANES, LANES).T
        return carry

    lax.fori_loop(0, WIN_ROWS, turn_given, 0)

    weight = wall[...].astype(F32).reshape(LANES, LANES).astype(BF16)
    bias = bias_ref[...]
    band = 2 * z + home

    firsts = 4 * (f % 8) + 2 * core
    rows = [
        jnp.clip(rows_ref[band * TILES + firsts + tile] - band * TILES, 0, TILES - 1) for tile in range(2)
    ]

    def add(k, totals):
        done = []
        for tile in range(2):
            near = jnp.where(home == core, nb_own[k, rows[tile]], nb_other[k, rows[tile]])
            place = (near // 8 - (dest_row - 2)) * WIN_COLS + near % 8 - 2 * half
            place = jnp.clip(place, 0, WIN_ROWS * WIN_COLS - 1)
            done.append(totals[tile] + jnp.dot(
                jnp.concatenate([feats_t[0, place], feats_t[1, place]], axis=1), mask[tile, k],
                preferred_element_type=F32,
            ))
        return tuple(done)

    zero = jnp.zeros((LANES + 16, CELLS), F32)
    totals = lax.fori_loop(0, SLOTS, add, (zero, zero), unroll=True)
    for tile in range(2):
        total = totals[tile].T
        base = win[2, 4 * half + 2 * core + tile - 2 * half].reshape(CELLS, LANES).astype(F32)
        degree = total[:, LANES : LANES + 1]
        normed = ((total[:, :LANES] + base) / jnp.sqrt(degree + 1.0)).astype(BF16)
        linear = jnp.dot(normed, weight, preferred_element_type=F32) + bias
        stage_o[tile] = (base + jnp.maximum(linear, 0.0)).astype(BF16)

    first_out = 4 * (f % 8) + 2 * core

    for i, chip in enumerate(chips):
        cells = pl.ds(pl.multiple_of(chip * CHUNK, CHUNK), CHUNK)
        copy = pltpu.make_async_remote_copy(
            stage_o.at[:, cells], obuf.at[pl.ds(first_out, 2)],
            out_send, out_sem,
            device_id=device(2 * z + home, chip), device_id_type=MESH,
        )
        sent = home != core if STEPS[i] == (0, 0) else True
        if sent is True:
            copy.start()
        else:
            pl.when(sent)(copy.start)

    @pl.when(home == core)
    def _():
        obuf[pl.ds(first_out, 2)] = stage_o[:, my_cells]

    nb_copy.wait_send()
    settle(weight_send, wall.at[pl.ds(0, 15)])
    for i in range(2):
        settle_count(to_y_send.at[i], first_y[i], 3, lambda n: relay_y.at[0, :, pl.ds(0, n)])
    settle(to_x_send, relay_x.at[:, :, pl.ds(0, 3)])
    settle_count(win_y_send, second_y, 16, lambda n: words_v.at[pl.ds(0, 2 * n)])
    settle_count(win_x_send, second_x, 8, lambda n: words_v.at[pl.ds(0, 4 * n)])
    settle_count(
        fwd_send, [row_exists(w) for w in range(WIN_ROWS)], WIN_ROWS, lambda n: win.at[pl.ds(0, n), :, kept]
    )

    @pl.when(home == core)
    def _():
        settle(word_send, stage_w.at[pl.ds(0, 30)])
        settle(out_send, obuf.at[pl.ds(0, 30)])

    @pl.when(home != core)
    def _():
        settle(word_send, stage_w)
        settle(out_send, obuf)

    @pl.when(home == core)
    def _():
        settle(out_sem, obuf.at[pl.ds(0, 30)])

    @pl.when(home != core)
    def _():
        settle(out_sem, obuf)

    def put(r, carry):
        out_ref[r] = obuf[inverse[r]]
        return carry

    lax.fori_loop(0, TILES, put, 0)


def solution(mesh):
    n_tiles = mesh.shape["tiles"]

    def per_device(feats, weight, bias, neighbours, counts, adj_words, tile_row):
        vmem = pl.BlockSpec(memory_space=pltpu.VMEM)
        hbm = pl.BlockSpec(memory_space=pl.ANY)
        words = adj_words.reshape(TILES, WORDS, CELLS)
        return pl.pallas_call(
            functools.partial(kernel, n_tiles),
            out_shape=pltpu.VMEM(feats.shape, BF16),
            in_specs=[hbm] * 7,
            out_specs=vmem,
            scratch_shapes=[
                pltpu.VMEM((TILES, CHUNK, LANES), BF16),
                pltpu.VMEM((TILES, WORDS, CELLS), I32),
                pltpu.VMEM((8, LANES), BF16),
                pltpu.VMEM((1, LANES), F32),
                pltpu.SMEM((TILES,), I32),
                pltpu.SMEM((n_tiles * TILES,), I32),
                pltpu.SMEM((SLOTS, TILES), I32),
                pltpu.SMEM((SLOTS, TILES), I32),
                pltpu.VMEM((4, 8, CHUNK, LANES), BF16),
                pltpu.VMEM((TILES, WORDS, LANES), I32),
                pltpu.VMEM((2, 8, 4, CHUNK, LANES), BF16),
                pltpu.VMEM((2, WIN_COLS, 4, CHUNK, LANES), BF16),
                pltpu.VMEM((WIN_ROWS, WIN_COLS, 4, 4, CHUNK, LANES), BF16),
                pltpu.VMEM((SLOTS, 2, WORDS, LANES), I32),
                pltpu.VMEM((16, 8, LANES), BF16),
                pltpu.VMEM((2, WORDS * BITS, LANES), I32),
                pltpu.VMEM((2, SLOTS, CELLS, CELLS), BF16),
                pltpu.VMEM((2, WIN_ROWS * WIN_COLS, LANES + 16, LANES), BF16),
                pltpu.VMEM((2, CELLS, LANES), BF16),
                pltpu.VMEM((TILES, CHUNK, LANES), BF16),
                pltpu.SMEM((TILES,), I32),
                pltpu.SemaphoreType.DMA((7,)),
                pltpu.SemaphoreType.REGULAR,
                pltpu.SemaphoreType.DMA,
                pltpu.SemaphoreType.DMA,
                pltpu.SemaphoreType.DMA,
                pltpu.SemaphoreType.DMA((4,)),
                pltpu.SemaphoreType.DMA,
                pltpu.SemaphoreType.DMA,
                pltpu.SemaphoreType.DMA((2,)),
                pltpu.SemaphoreType.DMA((2,)),
                pltpu.SemaphoreType.DMA,
                pltpu.SemaphoreType.DMA((2,)),
                pltpu.SemaphoreType.DMA,
                pltpu.SemaphoreType.DMA,
                pltpu.SemaphoreType.DMA((WIN_ROWS,)),
                pltpu.SemaphoreType.DMA,
                pltpu.SemaphoreType.DMA((WIN_ROWS,)),
                pltpu.SemaphoreType.DMA,
                pltpu.SemaphoreType.DMA,
            ],
            compiler_params=pltpu.CompilerParams(collective_id=0, has_side_effects=True),
        )(feats, weight, bias.reshape(1, LANES), neighbours.T, words, counts, tile_row)

    return jax.shard_map(
        per_device,
        mesh=mesh,
        in_specs=(
            P("tiles", "feat", None),
            P("feat", None),
            P(),
            P("tiles", None),
            P("tiles"),
            P("tiles", "feat", None, None),
            P(),
        ),
        out_specs=P("tiles", "feat", None),
        check_vma=False,
    )
```

```python
import functools

import jax
import jax.numpy as jnp
from jax import lax
from jax.experimental import pallas as pl
from jax.experimental.pallas import tpu as pltpu
from jax.sharding import PartitionSpec as P

MESH = pl.DeviceIdType.MESH
STEPS = (
    (2, 2), (1, 2), (3, 2), (2, 1), (2, 3), (0, 2), (2, 0), (1, 1),
    (3, 3), (1, 3), (3, 1), (0, 1), (0, 3), (1, 0), (3, 0), (0, 0),
)
BF16 = jnp.bfloat16
F32 = jnp.float32
I32 = jnp.int32

SLOTS = 16
CELLS = 256
CHUNK = 16
WORDS = 24
BITS = 11
LANES = 128
TILES = 32
WIN_ROWS = 5
WIN_COLS = 6


def kernel(
    n_tiles,
    feats_hbm, weight_hbm, bias_hbm, nb_hbm, words_hbm, counts_hbm, rows_hbm,
    out_ref,
    feats_v, words_v, weight_v, bias_ref, counts_ref, rows_ref, nb_own, nb_other, stage_f, stage_w, relay_y, relay_x, win, wbuf, wall, bits32, mask, feats_t, stage_o, obuf, inverse,
    local_sem, met_sem, nb_send, nb_sem, word_send, word_sem, weight_send, weight_sem, to_y_send, to_y_sem, to_x_send, to_x_sem, win_y_send, win_x_send, win_sem, fwd_send, fwd_sem, out_send, out_sem,
):
    t = lax.axis_index("tiles")
    f = lax.axis_index("feat")
    z = t // 2
    core = t % 2
    partner = 2 * z + 1 - core
    row_in_plane = f // 2
    y, x = f // 4, f % 4
    half = f % 2
    home = f // 8
    dest_row = 8 * z + row_in_plane
    n_planes = n_tiles // 2

    def device(tiles, feat):
        return {"tiles": tiles, "feat": feat}

    def settle(sem, piece):
        pltpu.make_async_copy(piece, piece, sem).wait()

    def settle_count(sem, sent, most, pieces):
        count = sum(jnp.asarray(one).astype(I32) for one in sent)
        for n in range(1, most + 1):

            @pl.when(count == n)
            def _():
                settle(sem, pieces(n))

    early = [
        pltpu.make_async_copy(rows_hbm, rows_ref, local_sem.at[0]),
        pltpu.make_async_copy(feats_hbm, feats_v, local_sem.at[1]),
    ]
    late = [
        pltpu.make_async_copy(words_hbm, words_v, local_sem.at[2]),
        pltpu.make_async_copy(counts_hbm, counts_ref, local_sem.at[3]),
        pltpu.make_async_copy(nb_hbm, nb_own, local_sem.at[4]),
        pltpu.make_async_copy(weight_hbm, weight_v, local_sem.at[5]),
        pltpu.make_async_copy(bias_hbm, bias_ref, local_sem.at[6]),
    ]
    for load in early:
        load.start()

    barrier = pltpu.get_barrier_semaphore()

    chips = [(f // 4 + dy) % 4 * 4 + (f % 4 + dx) % 4 for dy, dx in STEPS]

    for (dy, dx), chip in zip(STEPS, chips):
        if dy * dx == 0:
            for tiles in (partner,) if (dy, dx) == (0, 0) else (t, partner):
                pl.semaphore_signal(barrier, inc=1, device_id=device(tiles, chip), device_id_type=MESH)

    @pl.when(z > 0)
    def _():
        pl.semaphore_signal(barrier, inc=1, device_id=device(t - 2, f), device_id_type=MESH)

    @pl.when(z < n_planes - 1)
    def _():
        pl.semaphore_signal(barrier, inc=1, device_id=device(t + 2, f), device_id_type=MESH)

    for load in late:
        load.start()

    def plane_for(chip_y):
        below = jnp.logical_and(core == 0, chip_y == 3).astype(I32)
        above = jnp.logical_and(core == 1, chip_y == 0).astype(I32)
        return z - below + above

    def ahead_of(chip_y):
        return (2 * chip_y + jnp.where(core == 0, 2, 6)) % 8 - 2

    def in_slide(plane):
        return jnp.logical_and(plane >= 0, plane < n_planes)

    def row_exists(w):
        row = dest_row + w - 2
        return jnp.logical_and(row >= 0, row < 4 * n_tiles)

    def clear(w, carry):
        @pl.when(jnp.logical_not(row_exists(w)))
        def _():
            win[w] = jnp.zeros((WIN_COLS, 4, 2, 2, CHUNK, LANES), BF16)

        return carry

    lax.fori_loop(0, WIN_ROWS, clear, 0)

    ones_rows = jnp.ones((16, LANES), BF16)

    def fill_ones(i, carry):
        feats_t[0, i, pl.ds(LANES, 16)] = ones_rows
        feats_t[1, i, pl.ds(LANES, 16)] = ones_rows
        return carry

    lax.fori_loop(0, WIN_ROWS * WIN_COLS, fill_ones, 0)

    for load in early:
        load.wait()

    def own_row(s):
        return jnp.clip(rows_ref[t * TILES + s] - t * TILES, 0, TILES - 1)

    for s in range(TILES):
        stage_f[s // 8, s % 8] = feats_v[own_row(s)]

    at_end = jnp.logical_or(z == 0, z == n_planes - 1)

    @pl.when(at_end)
    def _():
        pl.semaphore_wait(barrier, 14)

    @pl.when(jnp.logical_not(at_end))
    def _():
        pl.semaphore_wait(barrier, 15)

    for step in (2, 1, 3):
        pl.semaphore_signal(
            met_sem, inc=1, device_id=device(t, (y + step) % 4 * 4 + x), device_id_type=MESH
        )

    @pl.when(jnp.logical_and(core == 0, z < n_planes - 1))
    def _():
        pl.semaphore_signal(met_sem, inc=1, device_id=device(t + 2, f), device_id_type=MESH)

    @pl.when(jnp.logical_and(core == 1, z > 0))
    def _():
        pl.semaphore_signal(met_sem, inc=1, device_id=device(t - 2, f), device_id_type=MESH)

    parity = (x + y) % 2
    first_y, first_x, second_y, second_x = ([], []), [], [], []

    def reaches(r, ahead):
        return jnp.logical_and(ahead >= r - 3, ahead <= r + 2)

    def send(copy, sent, sends):
        sends.append(sent)
        if sent is True:
            copy.start()
        else:
            pl.when(sent)(copy.start)

    def first_along_y(step, i, in_plane):
        to_y = (y + step) % 4
        plane = plane_for(to_y)
        sent = jnp.logical_and(in_slide(plane), reaches(2 * i + parity, ahead_of(to_y)))
        sent = jnp.logical_and(sent, (plane == z) == in_plane)
        if in_plane and step == 0:

            @pl.when(sent)
            def _():
                relay_y[i, :, y] = stage_f[2 * i + parity]

            return
        copy = pltpu.make_async_remote_copy(
            stage_f.at[2 * i + parity], relay_y.at[i, :, y], to_y_send.at[i], to_y_sem.at[i, y % 2],
            device_id=device(2 * plane + core, 4 * to_y + x), device_id_type=MESH,
        )
        send(copy, sent, first_y[i])

    for step in (2, 1, 3, 0):
        for i in range(2):
            first_along_y(step, i, True)
        to_x = (x + step) % 4
        for i in range(2):
            columns = pl.ds(2 * (to_x % 2), WIN_COLS)
            if step == 0:
                relay_x[i, :, x // 2, x % 2] = stage_f[2 * i + 1 - parity, columns]
            else:
                copy = pltpu.make_async_remote_copy(
                    stage_f.at[2 * i + 1 - parity, columns], relay_x.at[i, :, x // 2, x % 2],
                    to_x_send, to_x_sem.at[i, x % 2],
                    device_id=device(t, 4 * y + to_x), device_id_type=MESH,
                )
                send(copy, True, first_x)

    for load in late:
        load.wait()

    def order_words(s, carry):
        row = own_row(s)
        live = f < counts_ref[row]
        w = words_v[row]
        packed = w[:, :LANES] | (w[:, LANES:] << 16)
        stage_w[s] = jnp.where(live, packed, jnp.zeros_like(packed))
        return carry

    lax.fori_loop(0, TILES, order_words, 0)

    meets_beyond = jnp.where(core == 0, z > 0, z < n_planes - 1)

    @pl.when(meets_beyond)
    def _():
        pl.semaphore_wait(met_sem, 4)

    @pl.when(jnp.logical_not(meets_beyond))
    def _():
        pl.semaphore_wait(met_sem, 3)

    for step in (2, 1, 3, 0):
        for i in range(2):
            first_along_y(step, i, False)

    nb_copy = pltpu.make_async_remote_copy(
        nb_own, nb_other, nb_send, nb_sem, device_id=device(partner, f), device_id_type=MESH
    )
    nb_copy.start()

    word_sends = []
    for i, chip in enumerate(chips):
        for side in range(2):
            sent = chip // 8 == core
            if STEPS[i] == (0, 0):
                sent = jnp.logical_and(sent, side != core)
            copy = pltpu.make_async_remote_copy(
                stage_w.at[pl.ds(4 * (chip % 8) + 2 * side, 2)], wbuf.at[f],
                word_send, word_sem.at[f // 4],
                device_id=device(2 * z + side, chip), device_id_type=MESH,
            )
            word_sends.append(sent)
            pl.when(sent)(copy.start)

    @pl.when(home == core)
    def _():
        wbuf[f] = stage_w[pl.ds(4 * (f % 8) + 2 * core, 2)]

    weight_mine = weight_v[...]
    wall[f] = weight_mine

    def weight_copy(i):
        chip = (f + i) % 16
        return pltpu.make_async_remote_copy(
            weight_v, wall.at[f], weight_send, weight_sem,
            device_id=device(t, chip), device_id_type=MESH,
        )

    def start_weight(i, carry):
        weight_copy(i).start()
        return carry

    lax.fori_loop(1, 16, start_weight, 0)

    my_cells = pl.ds(pl.multiple_of(f * CHUNK, CHUNK), CHUNK)
    ahead = ahead_of(y)
    band_plane = z + jnp.logical_and(core == 0, y == 3).astype(I32) - jnp.logical_and(
        core == 1, y == 0).astype(I32)

    for i in range(2):
        for odd in range(2):
            r = 2 * i + (x + odd) % 2
            here = jnp.logical_and(in_slide(band_plane), reaches(r, ahead))
            own = jnp.logical_and(band_plane == z, y % 2 == odd)

            @pl.when(jnp.logical_and(here, jnp.logical_not(own)))
            def _():
                settle(to_y_sem.at[i, odd], relay_y.at[i, :, pl.ds(0, 2)])

            @pl.when(jnp.logical_and(here, own))
            def _():
                settle(to_y_sem.at[i, odd], relay_y.at[i, :, pl.ds(0, 1)])

            for step in (2, 1, 3, 0):
                to_x = (x + step) % 4
                gap = ahead + to_x // 2 - r
                w = jnp.clip(2 - gap, 0, WIN_ROWS - 1)
                columns = pl.ds(2 * (to_x % 2), WIN_COLS)
                needed = jnp.logical_and(here, jnp.logical_and(gap >= -2, gap <= 2))
                for q in range(2):
                    source_y = 2 * q + odd
                    sent = needed
                    if step == 0:
                        sent = jnp.logical_and(needed, core != q)

                        @pl.when(jnp.logical_and(needed, core == q))
                        def _():
                            win[w, :, source_y, x // 2, x % 2] = relay_y[i, columns, source_y]

                    copy = pltpu.make_async_remote_copy(
                        relay_y.at[i, columns, source_y], win.at[w, :, source_y, x // 2, x % 2],
                        win_y_send, win_sem.at[w],
                        device_id=device(2 * z + q, 4 * y + to_x), device_id_type=MESH,
                    )
                    send(copy, sent, second_y)

        for odd in range(2):
            r = 2 * i + 1 - (y + odd) % 2

            @pl.when(x % 2 == odd)
            def _():
                settle(to_x_sem.at[i, odd], relay_x.at[i, :, pl.ds(0, 1), odd])

            @pl.when(x % 2 != odd)
            def _():
                settle(to_x_sem.at[i, odd], relay_x.at[i, :, :, odd])

            for step in (2, 1, 3, 0):
                to_y = (y + step) % 4
                plane = plane_for(to_y)
                gap = ahead_of(to_y) + x // 2 - r
                w = jnp.clip(2 - gap, 0, WIN_ROWS - 1)
                sent = jnp.logical_and(in_slide(plane), jnp.logical_and(gap >= -2, gap <= 2))
                if step == 0:
                    at_home = jnp.logical_and(plane == z, home == core)
                    mine = jnp.logical_and(sent, at_home)
                    sent = jnp.logical_and(sent, jnp.logical_not(at_home))

                    @pl.when(mine)
                    def _():
                        win[w, :, y, :, odd] = relay_x[i, :, :, odd]

                copy = pltpu.make_async_remote_copy(
                    relay_x.at[i, :, :, odd], win.at[w, :, y, :, odd], win_x_send, win_sem.at[w],
                    device_id=device(2 * plane + home, 4 * to_y + x), device_id_type=MESH,
                )
                send(copy, sent, second_x)

    def unpack(k, carry):
        with_mine = jnp.logical_and(k == f // 4 * 4, core == home)

        @pl.when(with_mine)
        def _():
            settle(word_sem.at[k // 4], wbuf.at[pl.ds(k, 3)])

        @pl.when(jnp.logical_and(k % 4 == 0, jnp.logical_not(with_mine)))
        def _():
            settle(word_sem.at[k // 4], wbuf.at[pl.ds(k, 4)])

        for tile in range(2):
            packed = wbuf[k, tile]
            for b in range(BITS):
                bits32[0, pl.ds(b, WORDS, stride=BITS), :] = (packed >> b) & 1
                bits32[1, pl.ds(b, WORDS, stride=BITS), :] = (packed >> (16 + b)) & 1
            mask[tile, k, :, :LANES] = bits32[0, :CELLS].astype(F32).astype(BF16)
            mask[tile, k, :, LANES:] = bits32[1, :CELLS].astype(F32).astype(BF16)
        return carry

    lax.fori_loop(0, SLOTS, unpack, 0)

    nb_copy.wait_recv()

    settle(weight_sem, wall.at[pl.ds(0, 15)])
    kept = pl.ds(2 * core, 2)

    def forward_copy(w):
        return pltpu.make_async_remote_copy(
            win.at[w, :, kept], win.at[w, :, kept], fwd_send, fwd_sem.at[w],
            device_id=device(partner, f), device_id_type=MESH,
        )

    def forward(w, carry):
        from_here = (dest_row + w - 2) // 4 == t
        from_chip = (dest_row + w - 2) // 4 % 2 == core
        from_here = jnp.logical_and(from_here, home == core)

        @pl.when(jnp.logical_and(row_exists(w), jnp.logical_not(from_chip)))
        def _():
            settle(win_sem.at[w], words_v.at[pl.ds(0, 8)])

        @pl.when(jnp.logical_and(row_exists(w), jnp.logical_and(from_chip, jnp.logical_not(from_here))))
        def _():
            settle(win_sem.at[w], words_v.at[pl.ds(0, 7)])

        @pl.when(jnp.logical_and(row_exists(w), from_here))
        def _():
            settle(win_sem.at[w], words_v.at[pl.ds(0, 5)])

        @pl.when(row_exists(w))
        def _():
            forward_copy(w).start()

        return carry

    lax.fori_loop(0, WIN_ROWS, forward, 0)

    given = pl.ds(2 - 2 * core, 2)

    def turn_kept(w, carry):
        for c in range(WIN_COLS):
            feats_t[core, w * WIN_COLS + c, pl.ds(0, LANES)] = win[w, c, kept].reshape(LANES, LANES).T
        return carry

    lax.fori_loop(0, WIN_ROWS, turn_kept, 0)

    def turn_given(w, carry):
        @pl.when(row_exists(w))
        def _():
            forward_copy(w).wait_recv()

        for c in range(WIN_COLS):
            feats_t[1 - core, w * WIN_COLS + c, pl.ds(0, LANES)] = win[w, c, given].reshape(LANES, LANES).T
        return carry

    lax.fori_loop(0, WIN_ROWS, turn_given, 0)

    weight = wall[...].astype(F32).reshape(LANES, LANES).astype(BF16)
    bias = bias_ref[...]
    band = 2 * z + home

    firsts = 4 * (f % 8) + 2 * core
    rows = [
        jnp.clip(rows_ref[band * TILES + firsts + tile] - band * TILES, 0, TILES - 1) for tile in range(2)
    ]

    def add(k, totals):
        done = []
        for tile in range(2):
            near = jnp.where(home == core, nb_own[k, rows[tile]], nb_other[k, rows[tile]])
            place = (near // 8 - (dest_row - 2)) * WIN_COLS + near % 8 - 2 * half
            place = jnp.clip(place, 0, WIN_ROWS * WIN_COLS - 1)
            done.append(totals[tile] + jnp.dot(
                jnp.concatenate([feats_t[0, place], feats_t[1, place]], axis=1), mask[tile, k],
                preferred_element_type=F32,
            ))
        return tuple(done)

    zero = jnp.zeros((LANES + 16, CELLS), F32)
    totals = lax.fori_loop(0, SLOTS, add, (zero, zero), unroll=True)
    for tile in range(2):
        total = totals[tile].T
        base = win[2, 4 * half + 2 * core + tile - 2 * half].reshape(CELLS, LANES).astype(F32)
        degree = total[:, LANES : LANES + 1]
        normed = ((total[:, :LANES] + base) / jnp.sqrt(degree + 1.0)).astype(BF16)
        linear = jnp.dot(normed, weight, preferred_element_type=F32) + bias
        stage_o[tile] = (base + jnp.maximum(linear, 0.0)).astype(BF16)

    first_out = 4 * (f % 8) + 2 * core

    for i, chip in enumerate(chips):
        cells = pl.ds(pl.multiple_of(chip * CHUNK, CHUNK), CHUNK)
        copy = pltpu.make_async_remote_copy(
            stage_o.at[:, cells], obuf.at[pl.ds(first_out, 2)],
            out_send, out_sem,
            device_id=device(2 * z + home, chip), device_id_type=MESH,
        )
        sent = home != core if STEPS[i] == (0, 0) else True
        if sent is True:
            copy.start()
        else:
            pl.when(sent)(copy.start)

    @pl.when(home == core)
    def _():
        obuf[pl.ds(first_out, 2)] = stage_o[:, my_cells]

    def invert(r, carry):
        found = 0
        for s in range(1, TILES):
            found = found + jnp.where(rows_ref[t * TILES + s] == t * TILES + r, s, 0)
        inverse[r] = jnp.clip(found, 0, TILES - 1)
        return carry

    lax.fori_loop(0, TILES, invert, 0)

    nb_copy.wait_send()
    settle(weight_send, wall.at[pl.ds(0, 15)])
    for i in range(2):
        settle_count(to_y_send.at[i], first_y[i], 3, lambda n: relay_y.at[0, :, pl.ds(0, n)])
    settle(to_x_send, words_v.at[pl.ds(0, 6)])
    settle_count(win_y_send, second_y, 28, lambda n: words_v.at[pl.ds(0, n)])
    settle_count(win_x_send, second_x, 10, lambda n: words_v.at[pl.ds(0, 2 * n)])
    settle_count(
        fwd_send, [row_exists(w) for w in range(WIN_ROWS)], WIN_ROWS, lambda n: win.at[pl.ds(0, n), :, kept]
    )

    @pl.when(home == core)
    def _():
        settle(word_send, stage_w.at[pl.ds(0, 30)])
        settle(out_send, obuf.at[pl.ds(0, 30)])

    @pl.when(home != core)
    def _():
        settle(word_send, stage_w)
        settle(out_send, obuf)

    @pl.when(home == core)
    def _():
        settle(out_sem, obuf.at[pl.ds(0, 30)])

    @pl.when(home != core)
    def _():
        settle(out_sem, obuf)

    def put(r, carry):
        out_ref[r] = obuf[inverse[r]]
        return carry

    lax.fori_loop(0, TILES, put, 0)


def solution(mesh):
    n_tiles = mesh.shape["tiles"]

    def per_device(feats, weight, bias, neighbours, counts, adj_words, tile_row):
        vmem = pl.BlockSpec(memory_space=pltpu.VMEM)
        hbm = pl.BlockSpec(memory_space=pl.ANY)
        words = adj_words.reshape(TILES, WORDS, CELLS)
        return pl.pallas_call(
            functools.partial(kernel, n_tiles),
            out_shape=pltpu.VMEM(feats.shape, BF16),
            in_specs=[hbm] * 7,
            out_specs=vmem,
            scratch_shapes=[
                pltpu.VMEM((TILES, CHUNK, LANES), BF16),
                pltpu.VMEM((TILES, WORDS, CELLS), I32),
                pltpu.VMEM((8, LANES), BF16),
                pltpu.VMEM((1, LANES), F32),
                pltpu.SMEM((TILES,), I32),
                pltpu.SMEM((n_tiles * TILES,), I32),
                pltpu.SMEM((SLOTS, TILES), I32),
                pltpu.SMEM((SLOTS, TILES), I32),
                pltpu.VMEM((4, 8, CHUNK, LANES), BF16),
                pltpu.VMEM((TILES, WORDS, LANES), I32),
                pltpu.VMEM((2, 8, 4, CHUNK, LANES), BF16),
                pltpu.VMEM((2, WIN_COLS, 2, 2, CHUNK, LANES), BF16),
                pltpu.VMEM((WIN_ROWS, WIN_COLS, 4, 2, 2, CHUNK, LANES), BF16),
                pltpu.VMEM((SLOTS, 2, WORDS, LANES), I32),
                pltpu.VMEM((16, 8, LANES), BF16),
                pltpu.VMEM((2, WORDS * BITS, LANES), I32),
                pltpu.VMEM((2, SLOTS, CELLS, CELLS), BF16),
                pltpu.VMEM((2, WIN_ROWS * WIN_COLS, LANES + 16, LANES), BF16),
                pltpu.VMEM((2, CELLS, LANES), BF16),
                pltpu.VMEM((TILES, CHUNK, LANES), BF16),
                pltpu.SMEM((TILES,), I32),
                pltpu.SemaphoreType.DMA((7,)),
                pltpu.SemaphoreType.REGULAR,
                pltpu.SemaphoreType.DMA,
                pltpu.SemaphoreType.DMA,
                pltpu.SemaphoreType.DMA,
                pltpu.SemaphoreType.DMA((4,)),
                pltpu.SemaphoreType.DMA,
                pltpu.SemaphoreType.DMA,
                pltpu.SemaphoreType.DMA((2,)),
                pltpu.SemaphoreType.DMA((2, 2)),
                pltpu.SemaphoreType.DMA,
                pltpu.SemaphoreType.DMA((2, 2)),
                pltpu.SemaphoreType.DMA,
                pltpu.SemaphoreType.DMA,
                pltpu.SemaphoreType.DMA((WIN_ROWS,)),
                pltpu.SemaphoreType.DMA,
                pltpu.SemaphoreType.DMA((WIN_ROWS,)),
                pltpu.SemaphoreType.DMA,
                pltpu.SemaphoreType.DMA,
            ],
            compiler_params=pltpu.CompilerParams(collective_id=0, has_side_effects=True),
        )(feats, weight, bias.reshape(1, LANES), neighbours.T, words, counts, tile_row)

    return jax.shard_map(
        per_device,
        mesh=mesh,
        in_specs=(
            P("tiles", "feat", None),
            P("feat", None),
            P(),
            P("tiles", None),
            P("tiles"),
            P("tiles", "feat", None, None),
            P(),
        ),
        out_specs=P("tiles", "feat", None),
        check_vma=False,
    )
```
